256 devices in a mesh: patch: 32 (over y, z), sub: 8 (over x, core).
Axes of the slice: x: 4, y: 4, z: 8, core: 2. Of those that a mesh axis runs over, the one named last changes fastest.
Arguments:
- heat: float32 [2097152], P(('patch', 'sub')), may hold values from -6 to 6
- basis: bfloat16 [9, 4194304], P(None, ('patch', 'sub')), may hold values from -3 to 3
- area: float32 [4194304], P(('patch', 'sub')), may hold values from 0.2 to 2
- corners: int32 [3, 4194304], P(None, ('patch', 'sub')), may hold values from 0 to 9215, as said below
- send_sub: int32 [16384], P(('patch', 'sub')), may hold values from 0 to 8191
- send_pat: int32 [4, 32768], P(None, ('patch', 'sub')), may hold values from 0 to 8191
- live_faces: int32 [256], P(('patch', 'sub')), may hold values from 12288 to 16384, as said below
Outputs:
- divergence: float32 [2097152], P(('patch', 'sub'))
The draws below stay inside these ranges and needn't reach their ends.
Inputs may be any that keep to these rules, and one draw needn't show every extreme that they name: Face slot f of a device lies in tile t = f // 128; each of its corners is either an owned position in [64 t - 128, 64 t + 128) or a remote position from 8192 + 256 (t mod (4)) up to 255 beyond that; every position of the device's table is read by some face of the device. `live_faces`: some device has all 16384 slots live.
All inputs are finite; a program needn't handle non-finite values.
Results may differ from the reference program's by a relative error of at most 0.0003.
Values sent between devices are 32-bit elements; how exact they have to be, the bound alone decides.
A program may use at most 64 MiB of HBM per device.

```python
import math
import jax
import jax.numpy as jnp
from jax import lax

V_DEV = 8192
F_DEV = 16384
S_SUB = 64
S_PAT = 128
RADIUS = 2
VERTS = 2097152
FACES = 4194304
GROUP_SENDS = 16384
PATCH_SENDS = 32768
N_PATCH = 32
N_SUB = 8


def draw_corners(key, part):
    devices = N_PATCH * N_SUB
    remote_len = N_SUB * S_SUB + 2 * RADIUS * S_PAT
    remote_win = min(256, remote_len)
    remote_blocks = remote_len // remote_win
    tiles = F_DEV // 128
    slot = jnp.arange(F_DEV).astype(jnp.int32)
    tile = slot // 128
    inner = slot % 128

    def one_device(device_key):
        keys = jax.random.split(device_key, 6)
        tile_keys = jax.random.split(keys[0], tiles)
        orders = jax.vmap(lambda single: jax.random.permutation(single, 64))(tile_keys).astype(jnp.int32)
        first = 64 * tile + orders[tile, inner % 64]
        lower = jnp.maximum(0, 64 * (tile - 2))
        upper = jnp.minimum(V_DEV, 64 * (tile + 2))
        near_one = jax.random.randint(keys[1], (F_DEV,), lower, upper).astype(jnp.int32)
        near_two = jax.random.randint(keys[2], (F_DEV,), lower, upper).astype(jnp.int32)
        remote_order = jax.random.permutation(keys[3], remote_win).astype(jnp.int32)
        counter = tile // remote_blocks * 32 + inner // 4
        remote_base = V_DEV + remote_win * (tile % remote_blocks)
        far_one = remote_base + remote_order[counter % remote_win]
        far_two = remote_base + jax.random.randint(keys[4], (F_DEV,), 0, remote_win).astype(jnp.int32)
        flagged = jax.random.randint(keys[5], (F_DEV,), 0, 8) == 0
        second = jnp.where(inner % 4 == 0, far_one, near_one)
        third = jnp.where(flagged, far_two, near_two)
        return jnp.stack([first, second, third]).astype(jnp.int32)
    device_keys = jax.random.split(jax.random.fold_in(key, 11), devices)
    positions = jax.vmap(one_device)(device_keys)
    return positions.transpose(1, 0, 2).reshape(3, devices * F_DEV).astype(jnp.int32)


def draw_live_faces(key, part):
    devices = N_PATCH * N_SUB
    first, second = jax.random.split(jax.random.fold_in(key, 23))
    counts = jax.random.randint(first, (devices,), 3 * F_DEV // 4, F_DEV + 1).astype(jnp.int32)
    fullest = jax.random.randint(second, (), 0, devices)
    return jnp.where(jnp.arange(devices) == fullest, F_DEV, counts).astype(jnp.int32)


def place_ends(array, own_key, smallest, top_value):
    longest = array.shape.index(max(array.shape))
    spots = []
    for shift in (0, 1):
        where = [jax.random.randint(jax.random.fold_in(own_key, axis), (), 0, length) for axis, length in enumerate(array.shape)]
        where[longest] = (where[longest] + shift) % array.shape[longest]
        spots.append(tuple(where))
    return array.at[spots[0]].set(smallest).at[spots[1]].set(top_value)


def shard_levels(own_key, extent, cuts, least, top_value):
    factor_of, own = 1.0, jax.random.fold_in(own_key, 6)
    for position, shards_of in cuts:
        steps = jnp.exp(jax.random.uniform(jax.random.fold_in(own, position), (shards_of,), jnp.float32, least / len(cuts), top_value / len(cuts)))
        factor_of = factor_of * jnp.repeat(steps, extent[position] // shards_of).reshape([-1 if axis == position else 1 for axis in range(len(extent))])
    return factor_of


def centred(rng, dims, scale, bound, shards=(), dtype=jnp.bfloat16):
    level = shard_levels(rng, dims, shards, -0.22, 0.18) if shards else 1.0
    values = jax.random.normal(rng, dims, jnp.float32) * scale * level
    return jnp.minimum(jnp.maximum(values, -bound), bound).astype(dtype)


def setup_inputs(seed: int = 0) -> dict:
    splits = jax.random.split(jax.random.key(seed), 8)
    return {
        "heat": centred(splits[0], (VERTS,), 1.0, 6.0, ((0, 256),), jnp.float32),
        "basis": centred(splits[1], (9, FACES), 0.5, 3.0, ((1, 256),)),
        "area": jnp.clip(jnp.exp(math.log(2.0) - 2.3025851 * jax.random.uniform(splits[2], (FACES,), jnp.float32) ** shard_levels(splits[2], (FACES,), ((0, 256),), -0.2, 0.2)), 0.2, 2.0),
        "corners": draw_corners(jax.random.fold_in(splits[7], 71), 0),
        "send_sub": place_ends(jax.random.randint(splits[4], (GROUP_SENDS,), 0, V_DEV), jax.random.fold_in(splits[4], 1), 0, V_DEV - 1).astype(jnp.int32),
        "send_pat": place_ends(jax.random.randint(splits[5], (2 * RADIUS, PATCH_SENDS), 0, V_DEV), jax.random.fold_in(splits[5], 1), 0, V_DEV - 1).astype(jnp.int32),
        "live_faces": draw_live_faces(jax.random.fold_in(splits[7], 71), 0),
    }


def offset_list():
    return [k + 1 for k in range(RADIUS)] + [-(k + 1) for k in range(RADIUS)]

def face_terms(lookup_table, corner_ids, basis_dev, area_dev, live_count):
    slots = corner_ids.shape[1]
    values = lookup_table[corner_ids]
    gradients = basis_dev.astype(jnp.float32).reshape(3, 3, slots)
    gradient = lax.optimization_barrier(jnp.sum(gradients * values[:, None, :], axis=0))
    length = jnp.sqrt(lax.optimization_barrier(jnp.sum(gradient * gradient, axis=0)))
    field = -gradient / jnp.maximum(length, 1.0)
    projected = lax.optimization_barrier(jnp.sum(gradients * field[None, :, :], axis=1))
    live_mask = jnp.arange(slots) < live_count
    weight = jnp.where(live_mask, area_dev, 0.0)
    terms = projected * weight[None, :]
    empty = jnp.zeros((lookup_table.shape[0],), jnp.float32)
    return empty.at[corner_ids.reshape(-1)].add(terms.reshape(-1))

def reference(heat, basis, area, corners, send_sub, send_pat, live_faces):
    patch_count = N_PATCH
    sub_count = N_SUB
    devices = patch_count * sub_count
    owned_heat = heat.reshape(patch_count, sub_count, V_DEV)
    group_lists = send_sub.reshape(patch_count, sub_count, S_SUB)
    group_values = jnp.take_along_axis(owned_heat, group_lists, axis=2).reshape(patch_count, 1, sub_count * S_SUB)
    group_values = jnp.broadcast_to(group_values, (patch_count, sub_count, sub_count * S_SUB))
    patch_lists = send_pat.reshape(2 * RADIUS, patch_count, sub_count, S_PAT)
    blocks = []
    for block_index, offset in enumerate(offset_list()):
        sent = jnp.take_along_axis(owned_heat, patch_lists[block_index], axis=2)
        blocks.append(jnp.roll(sent, offset, axis=0))
    patch_values = jnp.stack(blocks, axis=2).reshape(patch_count, sub_count, 2 * RADIUS * S_PAT)
    lookup_table = jnp.concatenate([owned_heat, group_values, patch_values], axis=2)
    table_len = lookup_table.shape[2]
    lookup_table = lookup_table.reshape(devices, table_len)
    corner_ids = corners.reshape(3, devices, F_DEV).transpose(1, 0, 2)
    basis_dev = basis.reshape(9, devices, F_DEV).transpose(1, 0, 2)
    area_dev = area.reshape(devices, F_DEV)
    table_sums = lax.map(lambda pack: face_terms(*pack), (lookup_table, corner_ids, basis_dev, area_dev, live_faces))
    table_sums = table_sums.reshape(patch_count, sub_count, table_len)
    result = table_sums[:, :, :V_DEV]
    start = V_DEV
    group_sums = table_sums[:, :, start:start + sub_count * S_SUB].reshape(patch_count, sub_count, sub_count, S_SUB)
    group_sums = lax.optimization_barrier(jnp.sum(group_sums, axis=1))
    patch_ids = jnp.arange(patch_count).astype(jnp.int32)[:, None, None]
    sub_ids = jnp.arange(sub_count).astype(jnp.int32)[None, :, None]
    result = result.at[patch_ids, sub_ids, group_lists].add(group_sums)
    start = V_DEV + sub_count * S_SUB
    patch_sums = table_sums[:, :, start:].reshape(patch_count, sub_count, 2 * RADIUS, S_PAT)
    for block_index, offset in enumerate(offset_list()):
        returned = jnp.roll(patch_sums[:, :, block_index], -offset, axis=0)
        result = result.at[patch_ids, sub_ids, patch_lists[block_index]].add(returned)
    return result.reshape(-1)
```

```python
import functools

import jax
import jax.numpy as jnp
from jax import lax
from jax.experimental import pallas as pl
from jax.experimental.pallas import tpu as pltpu
from jax.sharding import PartitionSpec as P

RADIUS = 2
OFFSETS = [k + 1 for k in range(RADIUS)] + [-(k + 1) for k in range(RADIUS)]
F32 = jnp.float32
BF16 = jnp.bfloat16
I32 = jnp.int32
NT = (((1,), (1,)), ((), ()))


def lanes_of(table, lane):
    return jnp.take_along_axis(table, lane, axis=1, mode="promise_in_bounds")


def iota(shape, dim):
    return lax.broadcasted_iota(I32, shape, dim)


def kernel(
    patches,
    subs,
    live_ref,
    heat_hbm,
    basis_hbm,
    area_hbm,
    corners_hbm,
    ssub_hbm,
    spat_hbm,
    out_ref,
    heat,
    basis,
    area,
    corners,
    ssub,
    spat,
    lists,
    ctile,
    btile,
    blast,
    rows,
    near,
    fwd_send,
    fwd_sub,
    fwd_pat,
    ret_send,
    ret_sub,
    ret_pat,
    in_sem,
    send_sem,
    recv_sem,
):
    p = lax.axis_index("patch")
    s = lax.axis_index("sub")
    owned = 8192

    cp_heat = pltpu.make_async_copy(heat_hbm, heat.at[pl.ds(8, 64)], in_sem.at[0])
    cp_ssub = pltpu.make_async_copy(ssub_hbm, ssub, in_sem.at[1])
    cp_spat = pltpu.make_async_copy(spat_hbm, spat, in_sem.at[2])
    cp_corners = pltpu.make_async_copy(corners_hbm, corners, in_sem.at[3])
    cp_basis = pltpu.make_async_copy(basis_hbm, basis, in_sem.at[4])
    cp_area = pltpu.make_async_copy(area_hbm, area, in_sem.at[5])
    copies = (cp_heat, cp_ssub, cp_spat, cp_corners, cp_basis, cp_area)
    for copy in copies:
        copy.start()

    def peer_sub(d):
        return {"patch": p, "sub": lax.rem(s + d, subs)}

    def peer_pat(offset):
        return {"patch": lax.rem(p + offset + patches, patches), "sub": s}

    barrier = pltpu.get_barrier_semaphore()
    for d in range(1, subs):
        pl.semaphore_signal(barrier, inc=1, device_id=peer_sub(d), device_id_type=pl.DeviceIdType.MESH)
    for offset in OFFSETS:
        pl.semaphore_signal(barrier, inc=1, device_id=peer_pat(offset), device_id_type=pl.DeviceIdType.MESH)

    heat[0:8, :] = jnp.zeros((8, 128), F32)
    heat[72:80, :] = jnp.zeros((8, 128), F32)
    for r in range(4):
        near[r, 0:8, :] = jnp.zeros((8, 128), F32)
        near[r, 264:272, :] = jnp.zeros((8, 128), F32)

    cp_heat.wait()
    cp_ssub.wait()
    cp_spat.wait()

    lists[0:4, :] = spat[...]
    one = ssub[...]
    lists[4:5, :] = jnp.concatenate([one, one], axis=1)
    sub8 = iota((8, 128), 0)
    picked = []
    for j in range(5):
        index = jnp.broadcast_to(lists[j : j + 1, :], (8, 128))
        lane = index & 127
        row = index >> 7
        total = jnp.zeros((8, 128), F32)
        for g in range(8):
            values = lanes_of(heat[8 + 8 * g : 16 + 8 * g, :], lane)
            total = jnp.where(row == sub8 + 8 * g, values, total)
        value = jnp.sum(total, axis=0, keepdims=True)
        fwd_send[j] = value
        picked.append(value)

    pl.semaphore_wait(barrier, subs - 1 + 2 * RADIUS)

    forward = []
    for j, offset in enumerate(OFFSETS):
        copy = pltpu.make_async_remote_copy(
            src_ref=fwd_send.at[j],
            dst_ref=fwd_pat.at[j],
            send_sem=send_sem.at[j],
            recv_sem=recv_sem.at[j],
            device_id=peer_pat(offset),
            device_id_type=pl.DeviceIdType.MESH,
        )
        copy.start()
        forward.append(copy)
    for d in range(1, subs):
        copy = pltpu.make_async_remote_copy(
            src_ref=fwd_send.at[4],
            dst_ref=fwd_sub.at[s],
            send_sem=send_sem.at[4 + d],
            recv_sem=recv_sem.at[4 + d],
            device_id=peer_sub(d),
            device_id_type=pl.DeviceIdType.MESH,
        )
        copy.start()
        forward.append(copy)
    fwd_sub[s] = picked[4]

    cp_corners.wait()
    cp_basis.wait()
    cp_area.wait()
    def relayout(j, carry):
        for r in range(4):
            col = pl.multiple_of(j * 512 + 128 * r, 128)
            row = pl.multiple_of(j * 8, 8)
            ctile[r, pl.ds(row, 3), :] = corners[:, pl.ds(col, 128)]
            block = basis[:, pl.ds(col, 128)].astype(F32)
            btile[r, pl.ds(row, 8), :] = block[0:8]
            blast[r, pl.ds(row, 1), :] = block[8:9]
        return carry

    lax.fori_loop(0, 32, relayout, 0)

    low64 = iota((8, 128), 1) < 64
    lane8 = iota((8, 128), 1)
    a16 = iota((16, 128), 0)
    b32 = iota((32, 128), 0)
    live = live_ref[0]

    def one_class(r, far0, far1):
        def one_group(g, far_sum):
            base = pl.multiple_of(g * 64, 64)
            first = 8 + 16 * g
            if r == 0:
                tab_a = heat[pl.ds(first - 1, 8, stride=2), :]
                tab_b = heat[pl.ds(first, 8, stride=2), :]
            elif r == 1:
                tab_a = jnp.where(low64, heat[pl.ds(first + 1, 8, stride=2), :], heat[pl.ds(first - 1, 8, stride=2), :])
                tab_b = heat[pl.ds(first, 8, stride=2), :]
            elif r == 2:
                tab_a = heat[pl.ds(first, 8, stride=2), :]
                tab_b = heat[pl.ds(first + 1, 8, stride=2), :]
            else:
                tab_a = jnp.where(low64, heat[pl.ds(first + 2, 8, stride=2), :], heat[pl.ds(first, 8, stride=2), :])
                tab_b = heat[pl.ds(first + 1, 8, stride=2), :]
            values = []
            for k in range(3):
                corner = ctile[r, pl.ds(base + k, 8, stride=8), :]
                lane = corner & 127
                odd = (corner >> 7) & 1
                is_far = corner >= owned
                owned_value = jnp.where(odd == (r >> 1), lanes_of(tab_b, lane), lanes_of(tab_a, lane))
                far_value = jnp.where(odd == 1, lanes_of(far1, lane), lanes_of(far0, lane))
                values.append(jnp.where(is_far, far_value, owned_value))
                start = jnp.where(is_far, 248 + 8 * r, sub8 * 8 + (64 * g + 2 * r - 4))
                rows[0, k] = ((corner >> 5) - start).astype(F32)
                rows[1, k] = (corner & 31).astype(F32)
            bas = [btile[r, pl.ds(base + i, 8, stride=8), :] for i in range(8)]
            bas.append(blast[r, pl.ds(base, 8, stride=8), :])
            grad = [bas[c] * values[0] + bas[3 + c] * values[1] + bas[6 + c] * values[2] for c in range(3)]
            length = jnp.sqrt(grad[0] * grad[0] + grad[1] * grad[1] + grad[2] * grad[2])
            slot = sub8 * 512 + lane8 + (4096 * g + 128 * r)
            weight = jnp.where(slot < live, area[pl.ds(32 * g + r, 8, stride=4), :], 0.0)
            scale = -weight / jnp.maximum(length, 1.0)
            for k in range(3):
                term = (bas[3 * k] * grad[0] + bas[3 * k + 1] * grad[1] + bas[3 * k + 2] * grad[2]) * scale
                high = term.astype(BF16).astype(F32)
                rows[2, k] = high
                rows[3, k] = term - high
            for i in range(8):
                left, right = [], []
                for k in range(3):
                    hit = jnp.broadcast_to(rows[0, k, i : i + 1, :], (16, 128)) == a16.astype(F32)
                    high = jnp.where(hit, jnp.broadcast_to(rows[2, k, i : i + 1, :], (16, 128)), 0.0)
                    low = jnp.where(hit, jnp.broadcast_to(rows[3, k, i : i + 1, :], (16, 128)), 0.0)
                    left.append(jnp.concatenate([high, low], axis=0).astype(BF16))
                    hit = jnp.broadcast_to(rows[1, k, i : i + 1, :], (32, 128)) == b32.astype(F32)
                    right.append(jnp.where(hit, 1.0, 0.0).astype(BF16))
                sums = lax.dot_general(
                    jnp.concatenate(left, axis=1), jnp.concatenate(right, axis=1), NT, preferred_element_type=F32
                )
                sums = sums[0:16] + sums[16:32]
                near[r, pl.ds(pl.multiple_of(8 + base + 8 * i, 8), 8), 0:32] = sums[0:8]
                far_sum = far_sum + sums[8:16]
            return far_sum

        return lax.fori_loop(0, 4, one_group, jnp.zeros((8, 32), F32))

    def to_rows(far_sum):
        wide = jnp.concatenate([far_sum, jnp.zeros((8, 96), F32)], axis=1)
        total = jnp.where((sub8 & 3) == 0, wide, 0.0)
        for w in range(1, 4):
            total = jnp.where((sub8 & 3) == w, pltpu.roll(wide, 32 * w, axis=1), total)
        return jnp.sum(total[0:4], axis=0, keepdims=True), jnp.sum(total[4:8], axis=0, keepdims=True)

    def wide_rows(row):
        return jnp.broadcast_to(row, (8, 128))

    for copy in forward[4:]:
        copy.wait()
    low_row = iota((1, 128), 1) < 64
    for r in range(2):
        far = []
        for q in range(2):
            far.append(wide_rows(jnp.where(low_row, fwd_sub[4 * r + 2 * q], fwd_sub[4 * r + 2 * q + 1])))
        top, bottom = to_rows(one_class(r, far[0], far[1]))
        ret_send[2 * r] = top
        ret_send[2 * r + 1] = bottom

    back = []
    for d in range(1, subs):
        to = lax.rem(s + d, subs)
        copy = pltpu.make_async_remote_copy(
            src_ref=ret_send.at[to // 2],
            dst_ref=ret_sub.at[s],
            send_sem=send_sem.at[16 + 4 + d],
            recv_sem=recv_sem.at[16 + 4 + d],
            device_id=peer_sub(d),
            device_id_type=pl.DeviceIdType.MESH,
        )
        copy.start()
        back.append(copy)
    ret_sub[s] = ret_send[s // 2]

    back_pat = []
    for r in range(2, 4):
        far = []
        for q in range(2):
            j = 2 * (r - 2) + q
            forward[j].wait()
            far.append(wide_rows(fwd_pat[j]))
        for q, row in enumerate(to_rows(one_class(r, far[0], far[1]))):
            j = 2 * (r - 2) + q
            ret_send[2 * r + q] = row
            copy = pltpu.make_async_remote_copy(
                src_ref=ret_send.at[2 * r + q],
                dst_ref=ret_pat.at[j],
                send_sem=send_sem.at[16 + j],
                recv_sem=recv_sem.at[16 + j],
                device_id=peer_pat(-OFFSETS[j]),
                device_id_type=pl.DeviceIdType.MESH,
            )
            copy.start()
            back_pat.append(copy)

    quarter = lane8 >> 5
    blocks = []
    for m in range(8):
        block = None
        for w in range(4):
            part = None
            for r in range(4):
                piece = near[r, pl.ds(32 * m + w + 12 - 2 * r, 8, stride=4), :]
                part = piece if part is None else part + piece
            if w:
                part = pltpu.roll(part, 32 * w, axis=1)
                block = jnp.where(quarter == w, part, block)
            else:
                block = part
        blocks.append(block)
    owned_sums = jnp.concatenate(blocks, axis=0)

    lane_hit, row_hit = [], []
    for j in range(5):
        index = lists[j : j + 1, :]
        lane_hit.append(jnp.where(jnp.broadcast_to(index & 127, (128, 128)) == iota((128, 128), 0), 1.0, 0.0).astype(BF16))
        row_hit.append(jnp.broadcast_to(index >> 7, (64, 128)) == iota((64, 128), 0))

    for copy in back:
        copy.wait()
    returned = None
    for s2 in range(subs):
        returned = ret_sub[s2] if returned is None else returned + ret_sub[s2]
    half = iota((1, 128), 1) >> 6
    returned = jnp.where(half == lax.rem(s, 2), returned, 0.0)
    for copy in back_pat:
        copy.wait()
    incoming = [ret_pat[j] for j in range(4)] + [returned]
    left = []
    for j in range(5):
        high = incoming[j].astype(BF16).astype(F32)
        low = incoming[j] - high
        left.append(
            jnp.concatenate(
                [
                    jnp.where(row_hit[j], jnp.broadcast_to(high, (64, 128)), 0.0),
                    jnp.where(row_hit[j], jnp.broadcast_to(low, (64, 128)), 0.0),
                ],
                axis=0,
            ).astype(BF16)
        )
    sums = lax.dot_general(
        jnp.concatenate(left, axis=1), jnp.concatenate(lane_hit, axis=1), NT, preferred_element_type=F32
    )
    out_ref[...] = owned_sums + (sums[0:64] + sums[64:128])


def per_device(patches, subs, heat, basis, area, corners, send_sub, send_pat, live_faces):
    hbm = pl.BlockSpec(memory_space=pl.ANY)
    out = pl.pallas_call(
        functools.partial(kernel, patches, subs),
        out_shape=jax.ShapeDtypeStruct((64, 128), F32),
        in_specs=[pl.BlockSpec(memory_space=pltpu.SMEM)] + [hbm] * 6,
        out_specs=pl.BlockSpec(memory_space=pltpu.VMEM),
        scratch_shapes=[
            pltpu.VMEM((80, 128), F32),
            pltpu.VMEM((9, 16384), BF16),
            pltpu.VMEM((128, 128), F32),
            pltpu.VMEM((3, 16384), I32),
            pltpu.VMEM((1, 64), I32),
            pltpu.VMEM((4, 128), I32),
            pltpu.VMEM((8, 128), I32),
            pltpu.VMEM((4, 256, 128), I32),
            pltpu.VMEM((4, 256, 128), F32),
            pltpu.VMEM((4, 256, 128), F32),
            pltpu.VMEM((4, 3, 8, 128), F32),
            pltpu.VMEM((4, 272, 128), F32),
            pltpu.VMEM((5, 1, 128), F32),
            pltpu.VMEM((8, 1, 128), F32),
            pltpu.VMEM((4, 1, 128), F32),
            pltpu.VMEM((8, 1, 128), F32),
            pltpu.VMEM((8, 1, 128), F32),
            pltpu.VMEM((4, 1, 128), F32),
            pltpu.SemaphoreType.DMA((6,)),
            pltpu.SemaphoreType.DMA((32,)),
            pltpu.SemaphoreType.DMA((32,)),
        ],
        compiler_params=pltpu.CompilerParams(collective_id=0, has_side_effects=True),
        name="divergence",
    )(
        live_faces,
        heat.reshape(64, 128),
        basis,
        area.reshape(128, 128),
        corners,
        send_sub.reshape(1, 64),
        send_pat,
    )
    return out.reshape(-1)


def solution(mesh):
    placed = (
        P(("patch", "sub")),
        P(None, ("patch", "sub")),
        P(("patch", "sub")),
        P(None, ("patch", "sub")),
        P(("patch", "sub")),
        P(None, ("patch", "sub")),
        P(("patch", "sub")),
    )
    return jax.shard_map(
        functools.partial(per_device, mesh.shape["patch"], mesh.shape["sub"]),
        mesh=mesh,
        in_specs=placed,
        out_specs=P(("patch", "sub")),
        check_vma=False,
    )
```

```python
import functools

import jax
import jax.numpy as jnp
from jax import lax
from jax.experimental import pallas as pl
from jax.experimental.pallas import tpu as pltpu
from jax.sharding import PartitionSpec as P

RADIUS = 2
OFFSETS = [k + 1 for k in range(RADIUS)] + [-(k + 1) for k in range(RADIUS)]
F32 = jnp.float32
BF16 = jnp.bfloat16
I32 = jnp.int32
NT = (((1,), (1,)), ((), ()))


def lanes_of(table, lane):
    return jnp.take_along_axis(table, lane, axis=1, mode="promise_in_bounds")


def iota(shape, dim):
    return lax.broadcasted_iota(I32, shape, dim)


def kernel(
    patches,
    subs,
    live_hbm,
    heat_hbm,
    basis_hbm,
    area_hbm,
    corners_hbm,
    ssub_hbm,
    spat_hbm,
    out_ref,
    live_ref,
    heat,
    basis,
    area,
    corners,
    ssub,
    spat,
    lists,
    ctile,
    btile,
    blast,
    cgrp,
    vgrp,
    bgrp,
    wgrp,
    rows,
    near,
    fwd_send,
    fwd_sub,
    fwd_pat,
    ret_send,
    ret_sub,
    ret_pat,
    in_sem,
    send_sem,
    recv_sem,
):
    p = lax.axis_index("patch")
    s = lax.axis_index("sub")
    owned = 8192

    def peer_sub(d):
        return {"patch": p, "sub": lax.rem(s + d, subs)}

    def peer_pat(offset):
        return {"patch": lax.rem(p + offset + patches, patches), "sub": s}

    barrier = pltpu.get_barrier_semaphore()
    for offset in OFFSETS:
        pl.semaphore_signal(barrier, inc=1, device_id=peer_pat(offset), device_id_type=pl.DeviceIdType.MESH)
    for d in range(1, subs):
        pl.semaphore_signal(barrier, inc=1, device_id=peer_sub(d), device_id_type=pl.DeviceIdType.MESH)

    cp_heat = pltpu.make_async_copy(heat_hbm, heat.at[pl.ds(8, 64)], in_sem.at[0])
    cp_ssub = pltpu.make_async_copy(ssub_hbm, ssub, in_sem.at[1])
    cp_spat = pltpu.make_async_copy(spat_hbm, spat, in_sem.at[2])
    cp_corners = pltpu.make_async_copy(corners_hbm, corners, in_sem.at[3])
    cp_basis = pltpu.make_async_copy(basis_hbm, basis, in_sem.at[4])
    cp_area = pltpu.make_async_copy(area_hbm, area, in_sem.at[5])
    cp_live = pltpu.make_async_copy(live_hbm, live_ref, in_sem.at[6])
    copies = (cp_heat, cp_ssub, cp_spat, cp_corners, cp_basis, cp_area, cp_live)
    for copy in copies:
        copy.start()

    heat[0:8, :] = jnp.zeros((8, 128), F32)
    heat[72:80, :] = jnp.zeros((8, 128), F32)
    for r in range(4):
        near[r, 0:8, :] = jnp.zeros((8, 128), F32)
        near[r, 264:272, :] = jnp.zeros((8, 128), F32)

    cp_heat.wait()
    cp_ssub.wait()
    cp_spat.wait()

    lists[0:4, :] = spat[...]
    one = ssub[...]
    lists[4:5, :] = jnp.concatenate([one, one], axis=1)
    sub8 = iota((8, 128), 0)
    picked = []
    for j in range(5):
        index = jnp.broadcast_to(lists[j : j + 1, :], (8, 128))
        lane = index & 127
        row = index >> 7
        total = jnp.zeros((8, 128), F32)
        for g in range(8):
            values = lanes_of(heat[8 + 8 * g : 16 + 8 * g, :], lane)
            total = jnp.where(row == sub8 + 8 * g, values, total)
        value = jnp.sum(total, axis=0, keepdims=True)
        fwd_send[j] = value
        picked.append(value)

    pl.semaphore_wait(barrier, subs - 1 + 2 * RADIUS)

    forward = []
    for j, offset in enumerate(OFFSETS):
        copy = pltpu.make_async_remote_copy(
            src_ref=fwd_send.at[j],
            dst_ref=fwd_pat.at[j],
            send_sem=send_sem.at[j],
            recv_sem=recv_sem.at[j],
            device_id=peer_pat(offset),
            device_id_type=pl.DeviceIdType.MESH,
        )
        copy.start()
        forward.append(copy)
    for d in range(1, subs):
        copy = pltpu.make_async_remote_copy(
            src_ref=fwd_send.at[4],
            dst_ref=fwd_sub.at[s],
            send_sem=send_sem.at[4 + d],
            recv_sem=recv_sem.at[4 + d],
            device_id=peer_sub(d),
            device_id_type=pl.DeviceIdType.MESH,
        )
        copy.start()
        forward.append(copy)
    fwd_sub[s] = picked[4]

    cp_corners.wait()
    cp_basis.wait()
    cp_area.wait()
    cp_live.wait()

    def relayout(j, carry):
        for r in range(4):
            col = pl.multiple_of(j * 512 + 128 * r, 128)
            row = pl.multiple_of(j * 8, 8)
            ctile[r, pl.ds(row, 3), :] = corners[:, pl.ds(col, 128)]
            block = basis[:, pl.ds(col, 128)].astype(F32)
            btile[r, pl.ds(row, 8), :] = block[0:8]
            blast[r, pl.ds(row, 1), :] = block[8:9]
        return carry

    lax.fori_loop(0, 32, relayout, 0)

    low64 = iota((8, 128), 1) < 64
    lane8 = iota((8, 128), 1)
    a16 = iota((16, 128), 0).astype(F32)
    b32 = iota((32, 128), 0).astype(F32)
    live = live_ref[0]

    def prepare(g, carry):
        base = pl.multiple_of(g * 64, 64)
        first = 8 + 16 * g
        for r in range(4):
            m = first + (r >> 1)
            tab_a = heat[pl.ds(m - 1, 8, stride=2), :]
            tab_b = heat[pl.ds(m, 8, stride=2), :]
            if r & 1:
                tab_a = jnp.where(low64, heat[pl.ds(m + 1, 8, stride=2), :], tab_a)
            for k in range(3):
                corner = ctile[r, pl.ds(base + k, 8, stride=8), :]
                lane = corner & 127
                odd = (corner >> 7) & 1
                cgrp[r, g, k] = corner
                vgrp[r, g, k] = jnp.where(odd == (r >> 1), lanes_of(tab_b, lane), lanes_of(tab_a, lane))
                start = jnp.where(corner >= owned, 248 + 8 * r, sub8 * 8 + (64 * g + 2 * r - 4))
                rows[r, g, 0, k] = ((corner >> 5) - start).astype(F32)
                rows[r, g, 1, k] = (corner & 31).astype(F32)
            for i in range(8):
                bgrp[r, g, i] = btile[r, pl.ds(base + i, 8, stride=8), :]
            bgrp[r, g, 8] = blast[r, pl.ds(base, 8, stride=8), :]
            slot = sub8 * 512 + lane8 + (4096 * g + 128 * r)
            wgrp[r, g] = jnp.where(slot < live, area[pl.ds(32 * g + r, 8, stride=4), :], 0.0)
        return carry

    lax.fori_loop(0, 4, prepare, 0)

    def one_class(r, far0, far1):
        for g in range(4):
            values = []
            for k in range(3):
                corner = cgrp[r, g, k]
                lane = corner & 127
                far_value = jnp.where(((corner >> 7) & 1) == 1, lanes_of(far1, lane), lanes_of(far0, lane))
                values.append(jnp.where(corner >= owned, far_value, vgrp[r, g, k]))
            bas = [bgrp[r, g, i] for i in range(9)]
            grad = [bas[c] * values[0] + bas[3 + c] * values[1] + bas[6 + c] * values[2] for c in range(3)]
            length = jnp.sqrt(grad[0] * grad[0] + grad[1] * grad[1] + grad[2] * grad[2])
            scale = -wgrp[r, g] / jnp.maximum(length, 1.0)
            for k in range(3):
                term = (bas[3 * k] * grad[0] + bas[3 * k + 1] * grad[1] + bas[3 * k + 2] * grad[2]) * scale
                high = term.astype(BF16).astype(F32)
                rows[r, g, 2, k] = high
                rows[r, g, 3, k] = term - high
        far_sum = jnp.zeros((8, 32), F32)
        for g in range(4):
            for i in range(8):
                left, right = [], []
                for k in range(3):
                    a_row, b_row, high, low = (rows[r, g, q, k, i : i + 1, :] for q in range(4))
                    hit = jnp.broadcast_to(a_row, (16, 128)) == a16
                    high = jnp.where(hit, jnp.broadcast_to(high, (16, 128)), 0.0)
                    low = jnp.where(hit, jnp.broadcast_to(low, (16, 128)), 0.0)
                    left.append(jnp.concatenate([high, low], axis=0).astype(BF16))
                    hit = jnp.broadcast_to(b_row, (32, 128)) == b32
                    right.append(jnp.where(hit, 1.0, 0.0).astype(BF16))
                sums = lax.dot_general(
                    jnp.concatenate(left, axis=1), jnp.concatenate(right, axis=1), NT, preferred_element_type=F32
                )
                sums = sums[0:16] + sums[16:32]
                near[r, pl.ds(8 + 64 * g + 8 * i, 8), 0:32] = sums[0:8]
                far_sum = far_sum + sums[8:16]
        return far_sum

    def to_rows(far_sum):
        wide = jnp.concatenate([far_sum, jnp.zeros((8, 96), F32)], axis=1)
        total = jnp.where((sub8 & 3) == 0, wide, 0.0)
        for w in range(1, 4):
            total = jnp.where((sub8 & 3) == w, pltpu.roll(wide, 32 * w, axis=1), total)
        return jnp.sum(total[0:4], axis=0, keepdims=True), jnp.sum(total[4:8], axis=0, keepdims=True)

    def wide_rows(row):
        return jnp.broadcast_to(row, (8, 128))

    back, back_pat = [], []

    def patch_class(r):
        far = []
        for q in range(2):
            forward[2 * (r - 2) + q].wait()
            far.append(wide_rows(fwd_pat[2 * (r - 2) + q]))
        for q, row in enumerate(to_rows(one_class(r, far[0], far[1]))):
            j = 2 * (r - 2) + q
            ret_send[2 * r + q] = row
            copy = pltpu.make_async_remote_copy(
                src_ref=ret_send.at[2 * r + q],
                dst_ref=ret_pat.at[j],
                send_sem=send_sem.at[16 + j],
                recv_sem=recv_sem.at[16 + j],
                device_id=peer_pat(-OFFSETS[j]),
                device_id_type=pl.DeviceIdType.MESH,
            )
            copy.start()
            back_pat.append(copy)

    def group_classes():
        low_row = iota((1, 128), 1) < 64
        for copy in forward[4:]:
            copy.wait()
        for r in range(2):
            far = []
            for q in range(2):
                far.append(wide_rows(jnp.where(low_row, fwd_sub[4 * r + 2 * q], fwd_sub[4 * r + 2 * q + 1])))
            top, bottom = to_rows(one_class(r, far[0], far[1]))
            ret_send[2 * r] = top
            ret_send[2 * r + 1] = bottom
        for d in range(1, subs):
            to = lax.rem(s + d, subs)
            copy = pltpu.make_async_remote_copy(
                src_ref=ret_send.at[to // 2],
                dst_ref=ret_sub.at[s],
                send_sem=send_sem.at[16 + 4 + d],
                recv_sem=recv_sem.at[16 + 4 + d],
                device_id=peer_sub(d),
                device_id_type=pl.DeviceIdType.MESH,
            )
            copy.start()
            back.append(copy)
        ret_sub[s] = ret_send[s // 2]

    patch_class(3)
    group_classes()
    patch_class(2)

    quarter = lane8 >> 5
    blocks = []
    for m in range(8):
        block = None
        for w in range(4):
            part = None
            for r in range(4):
                piece = near[r, pl.ds(32 * m + w + 12 - 2 * r, 8, stride=4), :]
                part = piece if part is None else part + piece
            if w:
                part = pltpu.roll(part, 32 * w, axis=1)
                block = jnp.where(quarter == w, part, block)
            else:
                block = part
        blocks.append(block)
    owned_sums = jnp.concatenate(blocks, axis=0)

    lane_hit, row_hit = [], []
    for j in range(5):
        index = lists[j : j + 1, :]
        lane_hit.append(jnp.where(jnp.broadcast_to(index & 127, (128, 128)) == iota((128, 128), 0), 1.0, 0.0).astype(BF16))
        row_hit.append(jnp.broadcast_to(index >> 7, (64, 128)) == iota((64, 128), 0))

    for copy in back:
        copy.wait()
    returned = None
    for s2 in range(subs):
        returned = ret_sub[s2] if returned is None else returned + ret_sub[s2]
    half = iota((1, 128), 1) >> 6
    returned = jnp.where(half == lax.rem(s, 2), returned, 0.0)
    for copy in back_pat:
        copy.wait()
    incoming = [ret_pat[j] for j in range(4)] + [returned]
    left = []
    for j in range(5):
        high = incoming[j].astype(BF16).astype(F32)
        low = incoming[j] - high
        left.append(
            jnp.concatenate(
                [
                    jnp.where(row_hit[j], jnp.broadcast_to(high, (64, 128)), 0.0),
                    jnp.where(row_hit[j], jnp.broadcast_to(low, (64, 128)), 0.0),
                ],
                axis=0,
            ).astype(BF16)
        )
    sums = lax.dot_general(
        jnp.concatenate(left, axis=1), jnp.concatenate(lane_hit, axis=1), NT, preferred_element_type=F32
    )
    out_ref[...] = owned_sums + (sums[0:64] + sums[64:128])


def per_device(patches, subs, heat, basis, area, corners, send_sub, send_pat, live_faces):
    hbm = pl.BlockSpec(memory_space=pl.ANY)
    out = pl.pallas_call(
        functools.partial(kernel, patches, subs),
        out_shape=pltpu.VMEM((64, 128), F32),
        in_specs=[hbm] * 7,
        out_specs=pl.BlockSpec(memory_space=pltpu.VMEM),
        scratch_shapes=[
            pltpu.SMEM((1,), I32),
            pltpu.VMEM((80, 128), F32),
            pltpu.VMEM((9, 16384), BF16),
            pltpu.VMEM((128, 128), F32),
            pltpu.VMEM((3, 16384), I32),
            pltpu.VMEM((1, 64), I32),
            pltpu.VMEM((4, 128), I32),
            pltpu.VMEM((8, 128), I32),
            pltpu.VMEM((4, 256, 128), I32),
            pltpu.VMEM((4, 256, 128), F32),
            pltpu.VMEM((4, 256, 128), F32),
            pltpu.VMEM((4, 4, 3, 8, 128), I32),
            pltpu.VMEM((4, 4, 3, 8, 128), F32),
            pltpu.VMEM((4, 4, 9, 8, 128), F32),
            pltpu.VMEM((4, 4, 8, 128), F32),
            pltpu.VMEM((4, 4, 4, 3, 8, 128), F32),
            pltpu.VMEM((4, 272, 128), F32),
            pltpu.VMEM((5, 1, 128), F32),
            pltpu.VMEM((8, 1, 128), F32),
            pltpu.VMEM((4, 1, 128), F32),
            pltpu.VMEM((8, 1, 128), F32),
            pltpu.VMEM((8, 1, 128), F32),
            pltpu.VMEM((4, 1, 128), F32),
            pltpu.SemaphoreType.DMA((7,)),
            pltpu.SemaphoreType.DMA((32,)),
            pltpu.SemaphoreType.DMA((32,)),
        ],
        compiler_params=pltpu.CompilerParams(
            collective_id=0, has_side_effects=True, vmem_limit_bytes=32 * 1024 * 1024
        ),
        name="divergence",
    )(
        live_faces,
        *(
            pltpu.with_memory_space_constraint(x, pltpu.HBM)
            for x in (
                heat.reshape(64, 128),
                basis,
                area.reshape(128, 128),
                corners,
                send_sub.reshape(1, 64),
                send_pat,
            )
        )
    )
    return out.reshape(-1)


def solution(mesh):
    placed = (
        P(("patch", "sub")),
        P(None, ("patch", "sub")),
        P(("patch", "sub")),
        P(None, ("patch", "sub")),
        P(("patch", "sub")),
        P(None, ("patch", "sub")),
        P(("patch", "sub")),
    )
    return jax.shard_map(
        functools.partial(per_device, mesh.shape["patch"], mesh.shape["sub"]),
        mesh=mesh,
        in_specs=placed,
        out_specs=P(("patch", "sub")),
        check_vma=False,
    )
```

```python
import functools

import jax
import jax.numpy as jnp
from jax import lax
from jax.experimental import pallas as pl
from jax.experimental.pallas import tpu as pltpu
from jax.sharding import PartitionSpec as P

RADIUS = 2
OFFSETS = [k + 1 for k in range(RADIUS)] + [-(k + 1) for k in range(RADIUS)]
F32 = jnp.float32
BF16 = jnp.bfloat16
I32 = jnp.int32
NT = (((1,), (1,)), ((), ()))
ROW = 8


def lanes_of(table, lane):
    return jnp.take_along_axis(table, lane, axis=1, mode="promise_in_bounds")


def iota(shape, dim):
    return lax.broadcasted_iota(I32, shape, dim)


def kernel(
    patches,
    subs,
    live_hbm,
    heat_hbm,
    basis_hbm,
    area_hbm,
    corners_hbm,
    ssub_hbm,
    spat_hbm,
    out_ref,
    live_ref,
    heat,
    basis,
    area,
    corners,
    ssub,
    spat,
    lists,
    ctile,
    btile,
    blast,
    cgrp,
    vgrp,
    bgrp,
    wgrp,
    rows,
    near,
    fwd_send,
    fwd_sub,
    fwd_pat,
    relay,
    ret_send,
    ret_sub,
    ret_pat,
    in_sem,
    send_sem,
    recv_sem,
):
    p = lax.axis_index("patch")
    s = lax.axis_index("sub")
    owned = 8192

    def peer_sub(d):
        return {"patch": p, "sub": lax.rem(s + d, subs)}

    def peer_pat(offset):
        return {"patch": lax.rem(p + offset + patches, patches), "sub": s}

    barrier = pltpu.get_barrier_semaphore()
    last_row = patches - ROW
    for offset in OFFSETS:
        to = p + offset
        if offset > 0:
            to = jnp.where(to >= patches, to - ROW, to)
        pl.semaphore_signal(
            barrier,
            inc=1,
            device_id={"patch": lax.rem(to + patches, patches), "sub": s},
            device_id_type=pl.DeviceIdType.MESH,
        )

    @pl.when((p >= last_row) & (p < last_row + RADIUS))
    def _():
        pl.semaphore_signal(
            barrier, inc=1, device_id={"patch": p - last_row, "sub": s}, device_id_type=pl.DeviceIdType.MESH
        )

    for d in range(1, subs):
        pl.semaphore_signal(barrier, inc=1, device_id=peer_sub(d), device_id_type=pl.DeviceIdType.MESH)

    cp_heat = pltpu.make_async_copy(heat_hbm, heat.at[pl.ds(8, 64)], in_sem.at[0])
    cp_ssub = pltpu.make_async_copy(ssub_hbm, ssub, in_sem.at[1])
    cp_spat = pltpu.make_async_copy(spat_hbm, spat, in_sem.at[2])
    cp_corners = pltpu.make_async_copy(corners_hbm, corners, in_sem.at[3])
    cp_basis = pltpu.make_async_copy(basis_hbm, basis, in_sem.at[4])
    cp_area = pltpu.make_async_copy(area_hbm, area, in_sem.at[5])
    cp_live = pltpu.make_async_copy(live_hbm, live_ref, in_sem.at[6])
    copies = (cp_heat, cp_ssub, cp_spat, cp_corners, cp_basis, cp_area, cp_live)
    for copy in copies:
        copy.start()

    heat[0:8, :] = jnp.zeros((8, 128), F32)
    heat[72:80, :] = jnp.zeros((8, 128), F32)
    for r in range(4):
        near[r, 0:8, :] = jnp.zeros((8, 128), F32)
        near[r, 264:272, :] = jnp.zeros((8, 128), F32)

    cp_heat.wait()
    cp_ssub.wait()
    cp_spat.wait()

    lists[0:4, :] = spat[...]
    one = ssub[...]
    lists[4:5, :] = jnp.concatenate([one, one], axis=1)
    sub8 = iota((8, 128), 0)
    picked = []
    for j in range(5):
        index = jnp.broadcast_to(lists[j : j + 1, :], (8, 128))
        lane = index & 127
        row = index >> 7
        total = jnp.zeros((8, 128), F32)
        for g in range(8):
            values = lanes_of(heat[8 + 8 * g : 16 + 8 * g, :], lane)
            total = jnp.where(row == sub8 + 8 * g, values, total)
        value = jnp.sum(total, axis=0, keepdims=True)
        fwd_send[j] = value
        picked.append(value)

    signals = subs - 1 + 2 * RADIUS
    for k in range(RADIUS):
        signals = signals + (RADIUS - k) * (p == last_row + k).astype(I32) - (RADIUS - 1 - k) * (p == k).astype(I32)
    pl.semaphore_wait(barrier, signals)

    forward, relays = [], []
    for j, offset in enumerate(OFFSETS):
        copy = pltpu.make_async_remote_copy(
            src_ref=fwd_send.at[j],
            dst_ref=fwd_pat.at[j],
            send_sem=send_sem.at[j],
            recv_sem=recv_sem.at[j],
            device_id=peer_pat(offset),
            device_id_type=pl.DeviceIdType.MESH,
        )
        forward.append(copy)
        if offset > 0:
            copy.start()
            continue
        slot = -offset - 1
        first = pltpu.make_async_remote_copy(
            src_ref=fwd_send.at[j],
            dst_ref=relay.at[slot],
            send_sem=send_sem.at[j],
            recv_sem=recv_sem.at[12 + slot],
            device_id=peer_pat(-ROW),
            device_id_type=pl.DeviceIdType.MESH,
        )
        second = pltpu.make_async_remote_copy(
            src_ref=relay.at[slot],
            dst_ref=fwd_pat.at[j],
            send_sem=send_sem.at[12 + slot],
            recv_sem=recv_sem.at[j],
            device_id=peer_pat(ROW + offset - patches),
            device_id_type=pl.DeviceIdType.MESH,
        )
        relays.append(((p >= last_row) & (p < last_row - offset), first, second))
        pl.when(p < -offset)(first.start)
        pl.when(p >= -offset)(copy.start)
    for d in range(1, subs):
        copy = pltpu.make_async_remote_copy(
            src_ref=fwd_send.at[4],
            dst_ref=fwd_sub.at[s],
            send_sem=send_sem.at[4 + d],
            recv_sem=recv_sem.at[4 + d],
            device_id=peer_sub(d),
            device_id_type=pl.DeviceIdType.MESH,
        )
        copy.start()
        forward.append(copy)
    for on, first, second in relays:

        @pl.when(on)
        def _(first=first, second=second):
            first.wait_recv()
            second.start()

    fwd_sub[s] = picked[4]

    cp_corners.wait()
    cp_basis.wait()
    cp_area.wait()
    cp_live.wait()

    def relayout(j, carry):
        for r in range(4):
            col = pl.multiple_of(j * 512 + 128 * r, 128)
            row = pl.multiple_of(j * 8, 8)
            ctile[r, pl.ds(row, 3), :] = corners[:, pl.ds(col, 128)]
            block = basis[:, pl.ds(col, 128)].astype(F32)
            btile[r, pl.ds(row, 8), :] = block[0:8]
            blast[r, pl.ds(row, 1), :] = block[8:9]
        return carry

    lax.fori_loop(0, 32, relayout, 0)

    low64 = iota((8, 128), 1) < 64
    lane8 = iota((8, 128), 1)
    a16 = iota((16, 128), 0).astype(F32)
    b32 = iota((32, 128), 0).astype(F32)
    live = live_ref[0]

    def prepare(g, carry):
        base = pl.multiple_of(g * 64, 64)
        first = 8 + 16 * g
        for r in range(4):
            m = first + (r >> 1)
            tab_a = heat[pl.ds(m - 1, 8, stride=2), :]
            tab_b = heat[pl.ds(m, 8, stride=2), :]
            if r & 1:
                tab_a = jnp.where(low64, heat[pl.ds(m + 1, 8, stride=2), :], tab_a)
            for k in range(3):
                corner = ctile[r, pl.ds(base + k, 8, stride=8), :]
                lane = corner & 127
                odd = (corner >> 7) & 1
                cgrp[r, g, k] = corner
                vgrp[r, g, k] = jnp.where(odd == (r >> 1), lanes_of(tab_b, lane), lanes_of(tab_a, lane))
                start = jnp.where(corner >= owned, 248 + 8 * r, sub8 * 8 + (64 * g + 2 * r - 4))
                rows[r, g, 0, k] = ((corner >> 5) - start).astype(F32)
                rows[r, g, 1, k] = (corner & 31).astype(F32)
            for i in range(8):
                bgrp[r, g, i] = btile[r, pl.ds(base + i, 8, stride=8), :]
            bgrp[r, g, 8] = blast[r, pl.ds(base, 8, stride=8), :]
            slot = sub8 * 512 + lane8 + (4096 * g + 128 * r)
            wgrp[r, g] = jnp.where(slot < live, area[pl.ds(32 * g + r, 8, stride=4), :], 0.0)
        return carry

    lax.fori_loop(0, 4, prepare, 0)

    def one_class(r, far0, far1):
        for g in range(4):
            values = []
            for k in range(3):
                corner = cgrp[r, g, k]
                lane = corner & 127
                far_value = jnp.where(((corner >> 7) & 1) == 1, lanes_of(far1, lane), lanes_of(far0, lane))
                values.append(jnp.where(corner >= owned, far_value, vgrp[r, g, k]))
            bas = [bgrp[r, g, i] for i in range(9)]
            grad = [bas[c] * values[0] + bas[3 + c] * values[1] + bas[6 + c] * values[2] for c in range(3)]
            length = jnp.sqrt(grad[0] * grad[0] + grad[1] * grad[1] + grad[2] * grad[2])
            scale = -wgrp[r, g] / jnp.maximum(length, 1.0)
            for k in range(3):
                term = (bas[3 * k] * grad[0] + bas[3 * k + 1] * grad[1] + bas[3 * k + 2] * grad[2]) * scale
                high = term.astype(BF16).astype(F32)
                rows[r, g, 2, k] = high
                rows[r, g, 3, k] = term - high
        far_sum = jnp.zeros((8, 32), F32)
        for g in range(4):
            for i in range(8):
                left, right = [], []
                for k in range(3):
                    a_row, b_row, high, low = (rows[r, g, q, k, i : i + 1, :] for q in range(4))
                    hit = jnp.broadcast_to(a_row, (16, 128)) == a16
                    high = jnp.where(hit, jnp.broadcast_to(high, (16, 128)), 0.0)
                    low = jnp.where(hit, jnp.broadcast_to(low, (16, 128)), 0.0)
                    left.append(jnp.concatenate([high, low], axis=0).astype(BF16))
                    hit = jnp.broadcast_to(b_row, (32, 128)) == b32
                    right.append(jnp.where(hit, 1.0, 0.0).astype(BF16))
                sums = lax.dot_general(
                    jnp.concatenate(left, axis=1), jnp.concatenate(right, axis=1), NT, preferred_element_type=F32
                )
                sums = sums[0:16] + sums[16:32]
                near[r, pl.ds(8 + 64 * g + 8 * i, 8), 0:32] = sums[0:8]
                far_sum = far_sum + sums[8:16]
        return far_sum

    def to_rows(far_sum):
        wide = jnp.concatenate([far_sum, jnp.zeros((8, 96), F32)], axis=1)
        total = jnp.where((sub8 & 3) == 0, wide, 0.0)
        for w in range(1, 4):
            total = jnp.where((sub8 & 3) == w, pltpu.roll(wide, 32 * w, axis=1), total)
        return jnp.sum(total[0:4], axis=0, keepdims=True), jnp.sum(total[4:8], axis=0, keepdims=True)

    def wide_rows(row):
        return jnp.broadcast_to(row, (8, 128))

    back, back_pat = [], []

    def patch_class(r):
        far = []
        for q in range(2):
            forward[2 * (r - 2) + q].wait()
            far.append(wide_rows(fwd_pat[2 * (r - 2) + q]))
        for q, row in enumerate(to_rows(one_class(r, far[0], far[1]))):
            j = 2 * (r - 2) + q
            ret_send[2 * r + q] = row
            copy = pltpu.make_async_remote_copy(
                src_ref=ret_send.at[2 * r + q],
                dst_ref=ret_pat.at[j],
                send_sem=send_sem.at[16 + j],
                recv_sem=recv_sem.at[16 + j],
                device_id=peer_pat(-OFFSETS[j]),
                device_id_type=pl.DeviceIdType.MESH,
            )
            copy.start()
            back_pat.append(copy)

    def group_classes():
        low_row = iota((1, 128), 1) < 64
        for copy in forward[4:]:
            copy.wait()
        for r in range(2):
            far = []
            for q in range(2):
                far.append(wide_rows(jnp.where(low_row, fwd_sub[4 * r + 2 * q], fwd_sub[4 * r + 2 * q + 1])))
            top, bottom = to_rows(one_class(r, far[0], far[1]))
            ret_send[2 * r] = top
            ret_send[2 * r + 1] = bottom
        for d in range(1, subs):
            to = lax.rem(s + d, subs)
            copy = pltpu.make_async_remote_copy(
                src_ref=ret_send.at[to // 2],
                dst_ref=ret_sub.at[s],
                send_sem=send_sem.at[16 + 4 + d],
                recv_sem=recv_sem.at[16 + 4 + d],
                device_id=peer_sub(d),
                device_id_type=pl.DeviceIdType.MESH,
            )
            copy.start()
            back.append(copy)
        ret_sub[s] = ret_send[s // 2]

    patch_class(3)
    group_classes()
    patch_class(2)

    quarter = lane8 >> 5
    blocks = []
    for m in range(8):
        block = None
        for w in range(4):
            part = None
            for r in range(4):
                piece = near[r, pl.ds(32 * m + w + 12 - 2 * r, 8, stride=4), :]
                part = piece if part is None else part + piece
            if w:
                part = pltpu.roll(part, 32 * w, axis=1)
                block = jnp.where(quarter == w, part, block)
            else:
                block = part
        blocks.append(block)
    owned_sums = jnp.concatenate(blocks, axis=0)

    lane_hit, row_hit = [], []
    for j in range(5):
        index = lists[j : j + 1, :]
        lane_hit.append(jnp.where(jnp.broadcast_to(index & 127, (128, 128)) == iota((128, 128), 0), 1.0, 0.0).astype(BF16))
        row_hit.append(jnp.broadcast_to(index >> 7, (64, 128)) == iota((64, 128), 0))

    for copy in back:
        copy.wait()
    returned = None
    for s2 in range(subs):
        returned = ret_sub[s2] if returned is None else returned + ret_sub[s2]
    half = iota((1, 128), 1) >> 6
    returned = jnp.where(half == lax.rem(s, 2), returned, 0.0)
    for copy in back_pat:
        copy.wait()
    for on, first, second in relays:
        pl.when(on)(second.wait_send)
    incoming = [ret_pat[j] for j in range(4)] + [returned]
    left = []
    for j in range(5):
        high = incoming[j].astype(BF16).astype(F32)
        low = incoming[j] - high
        left.append(
            jnp.concatenate(
                [
                    jnp.where(row_hit[j], jnp.broadcast_to(high, (64, 128)), 0.0),
                    jnp.where(row_hit[j], jnp.broadcast_to(low, (64, 128)), 0.0),
                ],
                axis=0,
            ).astype(BF16)
        )
    sums = lax.dot_general(
        jnp.concatenate(left, axis=1), jnp.concatenate(lane_hit, axis=1), NT, preferred_element_type=F32
    )
    out_ref[...] = owned_sums + (sums[0:64] + sums[64:128])


def per_device(patches, subs, heat, basis, area, corners, send_sub, send_pat, live_faces):
    hbm = pl.BlockSpec(memory_space=pl.ANY)
    out = pl.pallas_call(
        functools.partial(kernel, patches, subs),
        out_shape=pltpu.VMEM((64, 128), F32),
        in_specs=[hbm] * 7,
        out_specs=pl.BlockSpec(memory_space=pltpu.VMEM),
        scratch_shapes=[
            pltpu.SMEM((1,), I32),
            pltpu.VMEM((80, 128), F32),
            pltpu.VMEM((9, 16384), BF16),
            pltpu.VMEM((128, 128), F32),
            pltpu.VMEM((3, 16384), I32),
            pltpu.VMEM((1, 64), I32),
            pltpu.VMEM((4, 128), I32),
            pltpu.VMEM((8, 128), I32),
            pltpu.VMEM((4, 256, 128), I32),
            pltpu.VMEM((4, 256, 128), F32),
            pltpu.VMEM((4, 256, 128), F32),
            pltpu.VMEM((4, 4, 3, 8, 128), I32),
            pltpu.VMEM((4, 4, 3, 8, 128), F32),
            pltpu.VMEM((4, 4, 9, 8, 128), F32),
            pltpu.VMEM((4, 4, 8, 128), F32),
            pltpu.VMEM((4, 4, 4, 3, 8, 128), F32),
            pltpu.VMEM((4, 272, 128), F32),
            pltpu.VMEM((5, 1, 128), F32),
            pltpu.VMEM((8, 1, 128), F32),
            pltpu.VMEM((4, 1, 128), F32),
            pltpu.VMEM((RADIUS, 1, 128), F32),
            pltpu.VMEM((8, 1, 128), F32),
            pltpu.VMEM((8, 1, 128), F32),
            pltpu.VMEM((4, 1, 128), F32),
            pltpu.SemaphoreType.DMA((7,)),
            pltpu.SemaphoreType.DMA((32,)),
            pltpu.SemaphoreType.DMA((32,)),
        ],
        compiler_params=pltpu.CompilerParams(
            collective_id=0, has_side_effects=True, vmem_limit_bytes=32 * 1024 * 1024
        ),
        name="divergence",
    )(
        live_faces,
        *(
            pltpu.with_memory_space_constraint(x, pltpu.HBM)
            for x in (
                heat.reshape(64, 128),
                basis,
                area.reshape(128, 128),
                corners,
                send_sub.reshape(1, 64),
                send_pat,
            )
        )
    )
    return out.reshape(-1)


def solution(mesh):
    placed = (
        P(("patch", "sub")),
        P(None, ("patch", "sub")),
        P(("patch", "sub")),
        P(None, ("patch", "sub")),
        P(("patch", "sub")),
        P(None, ("patch", "sub")),
        P(("patch", "sub")),
    )
    return jax.shard_map(
        functools.partial(per_device, mesh.shape["patch"], mesh.shape["sub"]),
        mesh=mesh,
        in_specs=placed,
        out_specs=P(("patch", "sub")),
        check_vma=False,
    )
```

```python
import functools

import jax
import jax.numpy as jnp
from jax import lax
from jax.experimental import pallas as pl
from jax.experimental.pallas import tpu as pltpu
from jax.sharding import PartitionSpec as P

RADIUS = 2
OFFSETS = [k + 1 for k in range(RADIUS)] + [-(k + 1) for k in range(RADIUS)]
F32 = jnp.float32
BF16 = jnp.bfloat16
I32 = jnp.int32
NT = (((1,), (1,)), ((), ()))
ROW = 8


def lanes_of(table, lane):
    return jnp.take_along_axis(table, lane, axis=1, mode="promise_in_bounds")


def iota(shape, dim):
    return lax.broadcasted_iota(I32, shape, dim)


def kernel(
    patches,
    subs,
    live_hbm,
    heat_hbm,
    basis_hbm,
    area_hbm,
    corners_hbm,
    ssub_hbm,
    spat_hbm,
    out_ref,
    live_ref,
    heat,
    basis,
    area,
    corners,
    ssub,
    spat,
    lists,
    ctile,
    btile,
    blast,
    cgrp,
    vgrp,
    bgrp,
    wgrp,
    rows,
    near,
    fwd_send,
    fwd_sub,
    fwd_pat,
    relay,
    ret_send,
    ret_sub,
    ret_pat,
    in_sem,
    send_sem,
    recv_sem,
):
    p = lax.axis_index("patch")
    s = lax.axis_index("sub")
    owned = 8192

    def peer_sub(d):
        return {"patch": p, "sub": lax.rem(s + d, subs)}

    def peer_pat(offset):
        return {"patch": lax.rem(p + offset + patches, patches), "sub": s}

    barrier = pltpu.get_barrier_semaphore()
    last_row = patches - ROW
    at = lax.rem(p, ROW)
    odd_core = lax.rem(s, 2)
    linked = s + 1 - odd_core
    for offset in OFFSETS:
        to, core = p + offset, s
        if offset > 0:
            to = jnp.where(to >= patches, to - ROW, to)
            core = jnp.where(p + offset >= patches, linked, s)
        pl.semaphore_signal(
            barrier,
            inc=1,
            device_id={"patch": lax.rem(to + patches, patches), "sub": core},
            device_id_type=pl.DeviceIdType.MESH,
        )

    @pl.when((p >= last_row) & (at < RADIUS) & (odd_core == 1))
    def _():
        for back_by in range(2):
            pl.semaphore_signal(
                barrier,
                inc=1,
                device_id={"patch": p - last_row, "sub": s - back_by},
                device_id_type=pl.DeviceIdType.MESH,
            )

    for d in range(1, subs):
        pl.semaphore_signal(barrier, inc=1, device_id=peer_sub(d), device_id_type=pl.DeviceIdType.MESH)

    cp_heat = pltpu.make_async_copy(heat_hbm, heat.at[pl.ds(8, 64)], in_sem.at[0])
    cp_ssub = pltpu.make_async_copy(ssub_hbm, ssub, in_sem.at[1])
    cp_spat = pltpu.make_async_copy(spat_hbm, spat, in_sem.at[2])
    cp_corners = pltpu.make_async_copy(corners_hbm, corners, in_sem.at[3])
    cp_basis = pltpu.make_async_copy(basis_hbm, basis, in_sem.at[4])
    cp_area = pltpu.make_async_copy(area_hbm, area, in_sem.at[5])
    cp_live = pltpu.make_async_copy(live_hbm, live_ref, in_sem.at[6])
    copies = (cp_heat, cp_ssub, cp_spat, cp_corners, cp_basis, cp_area, cp_live)
    for copy in copies:
        copy.start()

    heat[0:8, :] = jnp.zeros((8, 128), F32)
    heat[72:80, :] = jnp.zeros((8, 128), F32)
    for r in range(4):
        near[r, 0:8, :] = jnp.zeros((8, 128), F32)
        near[r, 264:272, :] = jnp.zeros((8, 128), F32)

    cp_heat.wait()
    cp_ssub.wait()
    cp_spat.wait()

    lists[0:4, :] = spat[...]
    one = ssub[...]
    lists[4:5, :] = jnp.concatenate([one, one], axis=1)
    sub8 = iota((8, 128), 0)
    picked = []
    for j in range(5):
        index = jnp.broadcast_to(lists[j : j + 1, :], (8, 128))
        lane = index & 127
        row = index >> 7
        total = jnp.zeros((8, 128), F32)
        for g in range(8):
            values = lanes_of(heat[8 + 8 * g : 16 + 8 * g, :], lane)
            total = jnp.where(row == sub8 + 8 * g, values, total)
        value = jnp.sum(total, axis=0, keepdims=True)
        fwd_send[j] = value
        picked.append(value)

    signals = subs - 1 + 2 * RADIUS
    for k in range(RADIUS):
        over = RADIUS - k
        here = (at == k).astype(I32)
        first_row = (p < ROW).astype(I32)
        signals = signals + here * first_row * (1 - over)
        signals = signals + here * (p >= last_row).astype(I32) * odd_core * 2 * over
    pl.semaphore_wait(barrier, signals)

    forward, relays = [], []
    for j, offset in enumerate(OFFSETS):
        copy = pltpu.make_async_remote_copy(
            src_ref=fwd_send.at[j],
            dst_ref=fwd_pat.at[j],
            send_sem=send_sem.at[j],
            recv_sem=recv_sem.at[j],
            device_id=peer_pat(offset),
            device_id_type=pl.DeviceIdType.MESH,
        )
        forward.append(copy)
        if offset > 0:
            copy.start()
            continue
        slot = -offset - 1
        over, via = at < -offset, p < -offset
        place = odd_core * RADIUS + slot
        first = pltpu.make_async_remote_copy(
            src_ref=fwd_send.at[j],
            dst_ref=relay.at[place],
            send_sem=send_sem.at[j],
            recv_sem=recv_sem.at[32 + place],
            device_id={"patch": lax.rem(p + last_row, patches), "sub": linked},
            device_id_type=pl.DeviceIdType.MESH,
        )
        pl.when(via)(first.start)
        pl.when(jnp.logical_not(via))(copy.start)
        for kind in range(2):
            on = (odd_core == 1) & over & (p >= last_row)
            place = kind * RADIUS + slot
            hop = {
                "src_ref": relay.at[place],
                "dst_ref": fwd_pat.at[j],
                "send_sem": send_sem.at[32 + place],
                "device_id": {
                    "patch": lax.rem(p + ROW + offset, patches),
                    "sub": s if kind == 1 else s - odd_core,
                },
                "device_id_type": pl.DeviceIdType.MESH,
            }
            taken = pltpu.make_async_remote_copy(**{**hop, "dst_ref": relay.at[place]}, recv_sem=recv_sem.at[32 + place])
            onward = pltpu.make_async_remote_copy(**hop, recv_sem=recv_sem.at[j])
            relays.append((on, taken, onward))
    for on, taken, onward in reversed(relays):

        @pl.when(on)
        def _(taken=taken, onward=onward):
            taken.wait_recv()
            onward.start()

    for d in range(1, subs):
        copy = pltpu.make_async_remote_copy(
            src_ref=fwd_send.at[4],
            dst_ref=fwd_sub.at[s],
            send_sem=send_sem.at[4 + d],
            recv_sem=recv_sem.at[4 + d],
            device_id=peer_sub(d),
            device_id_type=pl.DeviceIdType.MESH,
        )
        copy.start()
        forward.append(copy)
    fwd_sub[s] = picked[4]

    cp_corners.wait()
    cp_basis.wait()
    cp_area.wait()
    cp_live.wait()

    def relayout(j, carry):
        for r in range(4):
            col = pl.multiple_of(j * 512 + 128 * r, 128)
            row = pl.multiple_of(j * 8, 8)
            ctile[r, pl.ds(row, 3), :] = corners[:, pl.ds(col, 128)]
            block = basis[:, pl.ds(col, 128)].astype(F32)
            btile[r, pl.ds(row, 8), :] = block[0:8]
            blast[r, pl.ds(row, 1), :] = block[8:9]
        return carry

    lax.fori_loop(0, 32, relayout, 0)

    low64 = iota((8, 128), 1) < 64
    lane8 = iota((8, 128), 1)
    a8 = iota((8, 128), 0).astype(F32)
    b32 = iota((32, 128), 0).astype(F32)
    live = live_ref[0]

    def prepare(g, carry):
        base = pl.multiple_of(g * 64, 64)
        first = 8 + 16 * g
        for r in range(4):
            m = first + (r >> 1)
            tab_a = heat[pl.ds(m - 1, 8, stride=2), :]
            tab_b = heat[pl.ds(m, 8, stride=2), :]
            if r & 1:
                tab_a = jnp.where(low64, heat[pl.ds(m + 1, 8, stride=2), :], tab_a)
            for k in range(3):
                corner = ctile[r, pl.ds(base + k, 8, stride=8), :]
                lane = corner & 127
                odd = (corner >> 7) & 1
                cgrp[r, g, k] = corner
                vgrp[r, g, k] = jnp.where(odd == (r >> 1), lanes_of(tab_b, lane), lanes_of(tab_a, lane))
                start = jnp.where(corner >= owned, 248 + 8 * r, sub8 * 8 + (64 * g + 2 * r - 4))
                rows[r, g, 0, k] = ((corner >> 5) - start).astype(F32)
                rows[r, g, 1, k] = (corner & 31).astype(F32)
            for i in range(8):
                bgrp[r, g, i] = btile[r, pl.ds(base + i, 8, stride=8), :]
            bgrp[r, g, 8] = blast[r, pl.ds(base, 8, stride=8), :]
            slot = sub8 * 512 + lane8 + (4096 * g + 128 * r)
            wgrp[r, g] = jnp.where(slot < live, area[pl.ds(32 * g + r, 8, stride=4), :], 0.0)
        return carry

    lax.fori_loop(0, 4, prepare, 0)

    def term_rows(r, g, i, k, places):
        hit = jnp.broadcast_to(rows[r, g, 0, k, i : i + 1, :], (8, 128)) == places
        high = jnp.where(hit, jnp.broadcast_to(rows[r, g, 2, k, i : i + 1, :], (8, 128)), 0.0)
        low = jnp.where(hit, jnp.broadcast_to(rows[r, g, 3, k, i : i + 1, :], (8, 128)), 0.0)
        return jnp.concatenate([high, low], axis=0).astype(BF16)

    def lane_rows(r, g, i, k):
        hit = jnp.broadcast_to(rows[r, g, 1, k, i : i + 1, :], (32, 128)) == b32
        return jnp.where(hit, 1.0, 0.0).astype(BF16)

    def one_class(r, far0, far1):
        for g in range(4):
            values = []
            for k in range(3):
                corner = cgrp[r, g, k]
                lane = corner & 127
                far_value = jnp.where(((corner >> 7) & 1) == 1, lanes_of(far1, lane), lanes_of(far0, lane))
                values.append(jnp.where(corner >= owned, far_value, vgrp[r, g, k]))
            bas = [bgrp[r, g, i] for i in range(9)]
            grad = [bas[c] * values[0] + bas[3 + c] * values[1] + bas[6 + c] * values[2] for c in range(3)]
            length = jnp.sqrt(grad[0] * grad[0] + grad[1] * grad[1] + grad[2] * grad[2])
            scale = -wgrp[r, g] / jnp.maximum(length, 1.0)
            for k in range(3):
                term = (bas[3 * k] * grad[0] + bas[3 * k + 1] * grad[1] + bas[3 * k + 2] * grad[2]) * scale
                high = term.astype(BF16).astype(F32)
                rows[r, g, 2, k] = high
                rows[r, g, 3, k] = term - high
        far_sum = jnp.zeros((8, 32), F32)
        for g in range(4):
            left, right = [], []
            for i in range(8):
                for k in range(3):
                    left.append(term_rows(r, g, i, k, a8 + 8.0))
                    right.append(lane_rows(r, g, i, k))
            sums = lax.dot_general(
                jnp.concatenate(left, axis=1), jnp.concatenate(right, axis=1), NT, preferred_element_type=F32
            )
            far_sum = far_sum + (sums[0:8] + sums[8:16])
        return far_sum

    def near_group(g, carry):
        for r in range(4):
            for i in range(8):
                sums = lax.dot_general(
                    jnp.concatenate([term_rows(r, g, i, k, a8) for k in range(3)], axis=1),
                    jnp.concatenate([lane_rows(r, g, i, k) for k in range(3)], axis=1),
                    NT,
                    preferred_element_type=F32,
                )
                near[r, pl.ds(pl.multiple_of(8 + 64 * g + 8 * i, 8), 8), 0:32] = sums[0:8] + sums[8:16]
        return carry

    def to_rows(far_sum):
        wide = jnp.concatenate([far_sum, jnp.zeros((8, 96), F32)], axis=1)
        total = jnp.where((sub8 & 3) == 0, wide, 0.0)
        for w in range(1, 4):
            total = jnp.where((sub8 & 3) == w, pltpu.roll(wide, 32 * w, axis=1), total)
        return jnp.sum(total[0:4], axis=0, keepdims=True), jnp.sum(total[4:8], axis=0, keepdims=True)

    def wide_rows(row):
        return jnp.broadcast_to(row, (8, 128))

    back, back_pat = [], []

    def patch_class(r):
        far = []
        for q in range(2):
            forward[2 * (r - 2) + q].wait()
            far.append(wide_rows(fwd_pat[2 * (r - 2) + q]))
        for q, row in enumerate(to_rows(one_class(r, far[0], far[1]))):
            j = 2 * (r - 2) + q
            ret_send[2 * r + q] = row
            copy = pltpu.make_async_remote_copy(
                src_ref=ret_send.at[2 * r + q],
                dst_ref=ret_pat.at[j],
                send_sem=send_sem.at[16 + j],
                recv_sem=recv_sem.at[16 + j],
                device_id=peer_pat(-OFFSETS[j]),
                device_id_type=pl.DeviceIdType.MESH,
            )
            copy.start()
            back_pat.append(copy)

    def group_classes():
        low_row = iota((1, 128), 1) < 64
        for copy in forward[4:]:
            copy.wait()
        for r in range(2):
            far = []
            for q in range(2):
                far.append(wide_rows(jnp.where(low_row, fwd_sub[4 * r + 2 * q], fwd_sub[4 * r + 2 * q + 1])))
            top, bottom = to_rows(one_class(r, far[0], far[1]))
            ret_send[2 * r] = top
            ret_send[2 * r + 1] = bottom
        for d in range(1, subs):
            to = lax.rem(s + d, subs)
            copy = pltpu.make_async_remote_copy(
                src_ref=ret_send.at[to // 2],
                dst_ref=ret_sub.at[s],
                send_sem=send_sem.at[16 + 4 + d],
                recv_sem=recv_sem.at[16 + 4 + d],
                device_id=peer_sub(d),
                device_id_type=pl.DeviceIdType.MESH,
            )
            copy.start()
            back.append(copy)
        ret_sub[s] = ret_send[s // 2]

    patch_class(3)
    group_classes()
    patch_class(2)
    lax.fori_loop(0, 4, near_group, 0)

    quarter = lane8 >> 5
    blocks = []
    for m in range(8):
        block = None
        for w in range(4):
            part = None
            for r in range(4):
                piece = near[r, pl.ds(32 * m + w + 12 - 2 * r, 8, stride=4), :]
                part = piece if part is None else part + piece
            if w:
                part = pltpu.roll(part, 32 * w, axis=1)
                block = jnp.where(quarter == w, part, block)
            else:
                block = part
        blocks.append(block)
    owned_sums = jnp.concatenate(blocks, axis=0)

    lane_hit, row_hit = [], []
    for j in range(5):
        index = lists[j : j + 1, :]
        lane_hit.append(jnp.where(jnp.broadcast_to(index & 127, (128, 128)) == iota((128, 128), 0), 1.0, 0.0).astype(BF16))
        row_hit.append(jnp.broadcast_to(index >> 7, (64, 128)) == iota((64, 128), 0))

    for copy in back:
        copy.wait()
    returned = None
    for s2 in range(subs):
        returned = ret_sub[s2] if returned is None else returned + ret_sub[s2]
    half = iota((1, 128), 1) >> 6
    returned = jnp.where(half == lax.rem(s, 2), returned, 0.0)
    for copy in back_pat:
        copy.wait()
    for on, taken, onward in relays:
        pl.when(on)(onward.wait_send)
    incoming = [ret_pat[j] for j in range(4)] + [returned]
    left = []
    for j in range(5):
        high = incoming[j].astype(BF16).astype(F32)
        low = incoming[j] - high
        left.append(
            jnp.concatenate(
                [
                    jnp.where(row_hit[j], jnp.broadcast_to(high, (64, 128)), 0.0),
                    jnp.where(row_hit[j], jnp.broadcast_to(low, (64, 128)), 0.0),
                ],
                axis=0,
            ).astype(BF16)
        )
    sums = lax.dot_general(
        jnp.concatenate(left, axis=1), jnp.concatenate(lane_hit, axis=1), NT, preferred_element_type=F32
    )
    out_ref[...] = owned_sums + (sums[0:64] + sums[64:128])


def per_device(patches, subs, heat, basis, area, corners, send_sub, send_pat, live_faces):
    hbm = pl.BlockSpec(memory_space=pl.ANY)
    out = pl.pallas_call(
        functools.partial(kernel, patches, subs),
        out_shape=pltpu.VMEM((64, 128), F32),
        in_specs=[hbm] * 7,
        out_specs=pl.BlockSpec(memory_space=pltpu.VMEM),
        scratch_shapes=[
            pltpu.SMEM((1,), I32),
            pltpu.VMEM((80, 128), F32),
            pltpu.VMEM((9, 16384), BF16),
            pltpu.VMEM((128, 128), F32),
            pltpu.VMEM((3, 16384), I32),
            pltpu.VMEM((1, 64), I32),
            pltpu.VMEM((4, 128), I32),
            pltpu.VMEM((8, 128), I32),
            pltpu.VMEM((4, 256, 128), I32),
            pltpu.VMEM((4, 256, 128), F32),
            pltpu.VMEM((4, 256, 128), F32),
            pltpu.VMEM((4, 4, 3, 8, 128), I32),
            pltpu.VMEM((4, 4, 3, 8, 128), F32),
            pltpu.VMEM((4, 4, 9, 8, 128), F32),
            pltpu.VMEM((4, 4, 8, 128), F32),
            pltpu.VMEM((4, 4, 4, 3, 8, 128), F32),
            pltpu.VMEM((4, 272, 128), F32),
            pltpu.VMEM((5, 1, 128), F32),
            pltpu.VMEM((8, 1, 128), F32),
            pltpu.VMEM((4, 1, 128), F32),
            pltpu.VMEM((2 * RADIUS, 1, 128), F32),
            pltpu.VMEM((8, 1, 128), F32),
            pltpu.VMEM((8, 1, 128), F32),
            pltpu.VMEM((4, 1, 128), F32),
            pltpu.SemaphoreType.DMA((7,)),
            pltpu.SemaphoreType.DMA((40,)),
            pltpu.SemaphoreType.DMA((40,)),
        ],
        compiler_params=pltpu.CompilerParams(
            collective_id=0, has_side_effects=True, vmem_limit_bytes=32 * 1024 * 1024
        ),
        name="divergence",
    )(
        live_faces,
        *(
            pltpu.with_memory_space_constraint(x, pltpu.HBM)
            for x in (
                heat.reshape(64, 128),
                basis,
                area.reshape(128, 128),
                corners,
                send_sub.reshape(1, 64),
                send_pat,
            )
        )
    )
    return out.reshape(-1)


def solution(mesh):
    placed = (
        P(("patch", "sub")),
        P(None, ("patch", "sub")),
        P(("patch", "sub")),
        P(None, ("patch", "sub")),
        P(("patch", "sub")),
        P(None, ("patch", "sub")),
        P(("patch", "sub")),
    )
    return jax.shard_map(
        functools.partial(per_device, mesh.shape["patch"], mesh.shape["sub"]),
        mesh=mesh,
        in_specs=placed,
        out_specs=P(("patch", "sub")),
        check_vma=False,
    )
```

```python
import functools

import jax
import jax.numpy as jnp
from jax import lax
from jax.experimental import pallas as pl
from jax.experimental.pallas import tpu as pltpu
from jax.sharding import PartitionSpec as P

RADIUS = 2
OFFSETS = [k + 1 for k in range(RADIUS)] + [-(k + 1) for k in range(RADIUS)]
F32 = jnp.float32
BF16 = jnp.bfloat16
I32 = jnp.int32
NT = (((1,), (1,)), ((), ()))
ROW = 8


def lanes_of(table, lane):
    return jnp.take_along_axis(table, lane, axis=1, mode="promise_in_bounds")


def iota(shape, dim):
    return lax.broadcasted_iota(I32, shape, dim)


def kernel(
    patches,
    subs,
    live_hbm,
    heat_hbm,
    basis_hbm,
    area_hbm,
    corners_hbm,
    ssub_hbm,
    spat_hbm,
    out_ref,
    live_ref,
    heat,
    basis,
    area,
    corners,
    ssub,
    spat,
    lists,
    ctile,
    btile,
    blast,
    cgrp,
    vgrp,
    bgrp,
    wgrp,
    rows,
    near,
    fwd_send,
    fwd_sub,
    fwd_pat,
    relay,
    ret_send,
    ret_sub,
    ret_pat,
    in_sem,
    send_sem,
    recv_sem,
):
    p = lax.axis_index("patch")
    s = lax.axis_index("sub")
    owned = 8192

    def peer_sub(d):
        return {"patch": p, "sub": lax.rem(s + d, subs)}

    def peer_pat(offset):
        return {"patch": lax.rem(p + offset + patches, patches), "sub": s}

    barrier = pltpu.get_barrier_semaphore()
    last_row = patches - ROW
    at = lax.rem(p, ROW)
    odd_core = lax.rem(s, 2)
    linked = s + 1 - odd_core
    for offset in OFFSETS:
        to, core = p + offset, s
        if offset > 0:
            to = jnp.where(to >= patches, to - ROW, to)
            core = jnp.where(p + offset >= patches, linked, s)
        pl.semaphore_signal(
            barrier,
            inc=1,
            device_id={"patch": lax.rem(to + patches, patches), "sub": core},
            device_id_type=pl.DeviceIdType.MESH,
        )

    @pl.when((p >= last_row) & (at < RADIUS) & (odd_core == 1))
    def _():
        for back_by in range(2):
            pl.semaphore_signal(
                barrier,
                inc=1,
                device_id={"patch": p - last_row, "sub": s - back_by},
                device_id_type=pl.DeviceIdType.MESH,
            )

    for d in range(1, subs):
        pl.semaphore_signal(barrier, inc=1, device_id=peer_sub(d), device_id_type=pl.DeviceIdType.MESH)

    cp_heat = pltpu.make_async_copy(heat_hbm, heat.at[pl.ds(8, 64)], in_sem.at[0])
    cp_ssub = pltpu.make_async_copy(ssub_hbm, ssub, in_sem.at[1])
    cp_spat = pltpu.make_async_copy(spat_hbm, spat, in_sem.at[2])
    cp_corners = pltpu.make_async_copy(corners_hbm, corners, in_sem.at[3])
    cp_basis = pltpu.make_async_copy(basis_hbm, basis, in_sem.at[4])
    cp_area = pltpu.make_async_copy(area_hbm, area, in_sem.at[5])
    cp_live = pltpu.make_async_copy(live_hbm, live_ref, in_sem.at[6])
    copies = (cp_heat, cp_ssub, cp_spat, cp_corners, cp_basis, cp_area, cp_live)
    for copy in copies:
        copy.start()

    heat[0:8, :] = jnp.zeros((8, 128), F32)
    heat[72:80, :] = jnp.zeros((8, 128), F32)
    for r in range(4):
        near[r, 0:8, :] = jnp.zeros((8, 128), F32)
        near[r, 264:272, :] = jnp.zeros((8, 128), F32)

    cp_heat.wait()
    cp_ssub.wait()
    cp_spat.wait()

    lists[0:4, :] = spat[...]
    one = ssub[...]
    lists[4:5, :] = jnp.concatenate([one, one], axis=1)
    sub8 = iota((8, 128), 0)
    picked = []
    for j in range(5):
        index = jnp.broadcast_to(lists[j : j + 1, :], (8, 128))
        lane = index & 127
        row = index >> 7
        total = jnp.zeros((8, 128), F32)
        for g in range(8):
            values = lanes_of(heat[8 + 8 * g : 16 + 8 * g, :], lane)
            total = jnp.where(row == sub8 + 8 * g, values, total)
        value = jnp.sum(total, axis=0, keepdims=True)
        fwd_send[j] = value
        picked.append(value)

    signals = subs - 1 + 2 * RADIUS
    for k in range(RADIUS):
        over = RADIUS - k
        here = (at == k).astype(I32)
        first_row = (p < ROW).astype(I32)
        signals = signals + here * first_row * (1 - over)
        signals = signals + here * (p >= last_row).astype(I32) * odd_core * 2 * over
    pl.semaphore_wait(barrier, signals)

    forward, relays, starts = [], [], []
    for j, offset in enumerate(OFFSETS):
        copy = pltpu.make_async_remote_copy(
            src_ref=fwd_send.at[j],
            dst_ref=fwd_pat.at[j],
            send_sem=send_sem.at[j],
            recv_sem=recv_sem.at[j],
            device_id=peer_pat(offset),
            device_id_type=pl.DeviceIdType.MESH,
        )
        forward.append(copy)
        if offset > 0:
            starts.append(copy.start)
            continue
        slot = -offset - 1
        over, via = at < -offset, p < -offset
        place = odd_core * RADIUS + slot
        first = pltpu.make_async_remote_copy(
            src_ref=fwd_send.at[j],
            dst_ref=relay.at[place],
            send_sem=send_sem.at[j],
            recv_sem=recv_sem.at[32 + place],
            device_id={"patch": lax.rem(p + last_row, patches), "sub": linked},
            device_id_type=pl.DeviceIdType.MESH,
        )
        starts.append(functools.partial(pl.when(via), first.start))
        starts.append(functools.partial(pl.when(jnp.logical_not(via)), copy.start))
        for kind in range(2):
            on = (odd_core == 1) & over & (p >= last_row)
            place = kind * RADIUS + slot
            hop = {
                "src_ref": relay.at[place],
                "dst_ref": fwd_pat.at[j],
                "send_sem": send_sem.at[32 + place],
                "device_id": {
                    "patch": lax.rem(p + ROW + offset, patches),
                    "sub": s if kind == 1 else s - odd_core,
                },
                "device_id_type": pl.DeviceIdType.MESH,
            }
            taken = pltpu.make_async_remote_copy(**{**hop, "dst_ref": relay.at[place]}, recv_sem=recv_sem.at[32 + place])
            onward = pltpu.make_async_remote_copy(**hop, recv_sem=recv_sem.at[j])
            relays.append((on, taken, onward))
    for on, taken, onward in reversed(relays):

        @pl.when(on)
        def _(taken=taken, onward=onward):
            taken.wait_recv()
            onward.start()

    for start in reversed(starts):
        start()
    for d in range(1, subs):
        copy = pltpu.make_async_remote_copy(
            src_ref=fwd_send.at[4],
            dst_ref=fwd_sub.at[s],
            send_sem=send_sem.at[4 + d],
            recv_sem=recv_sem.at[4 + d],
            device_id=peer_sub(d),
            device_id_type=pl.DeviceIdType.MESH,
        )
        copy.start()
        forward.append(copy)
    fwd_sub[s] = picked[4]

    cp_corners.wait()
    cp_basis.wait()
    cp_area.wait()
    cp_live.wait()

    def relayout(j, carry):
        for r in range(4):
            col = pl.multiple_of(j * 512 + 128 * r, 128)
            row = pl.multiple_of(j * 8, 8)
            ctile[r, pl.ds(row, 3), :] = corners[:, pl.ds(col, 128)]
            block = basis[:, pl.ds(col, 128)].astype(F32)
            btile[r, pl.ds(row, 8), :] = block[0:8]
            blast[r, pl.ds(row, 1), :] = block[8:9]
        return carry

    lax.fori_loop(0, 32, relayout, 0)

    low64 = iota((8, 128), 1) < 64
    lane8 = iota((8, 128), 1)
    a8 = iota((8, 128), 0).astype(F32)
    b32 = iota((32, 128), 0).astype(F32)
    live = live_ref[0]

    def prepare(g, carry):
        base = pl.multiple_of(g * 64, 64)
        first = 8 + 16 * g
        for r in range(4):
            m = first + (r >> 1)
            tab_a = heat[pl.ds(m - 1, 8, stride=2), :]
            tab_b = heat[pl.ds(m, 8, stride=2), :]
            if r & 1:
                tab_a = jnp.where(low64, heat[pl.ds(m + 1, 8, stride=2), :], tab_a)
            for k in range(3):
                corner = ctile[r, pl.ds(base + k, 8, stride=8), :]
                lane = corner & 127
                odd = (corner >> 7) & 1
                cgrp[r, g, k] = corner
                vgrp[r, g, k] = jnp.where(odd == (r >> 1), lanes_of(tab_b, lane), lanes_of(tab_a, lane))
                start = jnp.where(corner >= owned, 248 + 8 * r, sub8 * 8 + (64 * g + 2 * r - 4))
                rows[r, g, 0, k] = ((corner >> 5) - start).astype(F32)
                rows[r, g, 1, k] = (corner & 31).astype(F32)
            for i in range(8):
                bgrp[r, g, i] = btile[r, pl.ds(base + i, 8, stride=8), :]
            bgrp[r, g, 8] = blast[r, pl.ds(base, 8, stride=8), :]
            slot = sub8 * 512 + lane8 + (4096 * g + 128 * r)
            wgrp[r, g] = jnp.where(slot < live, area[pl.ds(32 * g + r, 8, stride=4), :], 0.0)
        return carry

    lax.fori_loop(0, 4, prepare, 0)

    def term_rows(r, g, i, k, places):
        hit = jnp.broadcast_to(rows[r, g, 0, k, i : i + 1, :], (8, 128)) == places
        high = jnp.where(hit, jnp.broadcast_to(rows[r, g, 2, k, i : i + 1, :], (8, 128)), 0.0)
        low = jnp.where(hit, jnp.broadcast_to(rows[r, g, 3, k, i : i + 1, :], (8, 128)), 0.0)
        return jnp.concatenate([high, low], axis=0).astype(BF16)

    def lane_rows(r, g, i, k):
        hit = jnp.broadcast_to(rows[r, g, 1, k, i : i + 1, :], (32, 128)) == b32
        return jnp.where(hit, 1.0, 0.0).astype(BF16)

    def one_class(r, far0, far1):
        for g in range(4):
            values = []
            for k in range(3):
                corner = cgrp[r, g, k]
                lane = corner & 127
                far_value = jnp.where(((corner >> 7) & 1) == 1, lanes_of(far1, lane), lanes_of(far0, lane))
                values.append(jnp.where(corner >= owned, far_value, vgrp[r, g, k]))
            bas = [bgrp[r, g, i] for i in range(9)]
            grad = [bas[c] * values[0] + bas[3 + c] * values[1] + bas[6 + c] * values[2] for c in range(3)]
            square = grad[0] * grad[0] + grad[1] * grad[1] + grad[2] * grad[2]
            scale = -wgrp[r, g] * lax.rsqrt(jnp.maximum(square, 1.0))
            for k in range(3):
                term = (bas[3 * k] * grad[0] + bas[3 * k + 1] * grad[1] + bas[3 * k + 2] * grad[2]) * scale
                high = term.astype(BF16).astype(F32)
                rows[r, g, 2, k] = high
                rows[r, g, 3, k] = term - high
        far_sum = jnp.zeros((8, 32), F32)
        for g in range(4):
            left, right = [], []
            for i in range(8):
                for k in range(3):
                    left.append(term_rows(r, g, i, k, a8 + 8.0))
                    right.append(lane_rows(r, g, i, k))
            sums = lax.dot_general(
                jnp.concatenate(left, axis=1), jnp.concatenate(right, axis=1), NT, preferred_element_type=F32
            )
            far_sum = far_sum + (sums[0:8] + sums[8:16])
        return far_sum

    def near_group(g, carry):
        for r in range(4):
            for i in range(8):
                sums = lax.dot_general(
                    jnp.concatenate([term_rows(r, g, i, k, a8) for k in range(3)], axis=1),
                    jnp.concatenate([lane_rows(r, g, i, k) for k in range(3)], axis=1),
                    NT,
                    preferred_element_type=F32,
                )
                near[r, pl.ds(pl.multiple_of(8 + 64 * g + 8 * i, 8), 8), 0:32] = sums[0:8] + sums[8:16]
        return carry

    def to_rows(far_sum):
        wide = jnp.concatenate([far_sum, jnp.zeros((8, 96), F32)], axis=1)
        total = jnp.where((sub8 & 3) == 0, wide, 0.0)
        for w in range(1, 4):
            total = jnp.where((sub8 & 3) == w, pltpu.roll(wide, 32 * w, axis=1), total)
        return jnp.sum(total[0:4], axis=0, keepdims=True), jnp.sum(total[4:8], axis=0, keepdims=True)

    def wide_rows(row):
        return jnp.broadcast_to(row, (8, 128))

    back, back_pat = [], []

    def patch_class(r):
        far = []
        for q in range(2):
            forward[2 * (r - 2) + q].wait()
            far.append(wide_rows(fwd_pat[2 * (r - 2) + q]))
        for q, row in enumerate(to_rows(one_class(r, far[0], far[1]))):
            j = 2 * (r - 2) + q
            ret_send[2 * r + q] = row
            copy = pltpu.make_async_remote_copy(
                src_ref=ret_send.at[2 * r + q],
                dst_ref=ret_pat.at[j],
                send_sem=send_sem.at[16 + j],
                recv_sem=recv_sem.at[16 + j],
                device_id=peer_pat(-OFFSETS[j]),
                device_id_type=pl.DeviceIdType.MESH,
            )
            copy.start()
            back_pat.append(copy)

    def group_classes():
        low_row = iota((1, 128), 1) < 64
        for copy in forward[4:]:
            copy.wait()
        for r in range(2):
            far = []
            for q in range(2):
                far.append(wide_rows(jnp.where(low_row, fwd_sub[4 * r + 2 * q], fwd_sub[4 * r + 2 * q + 1])))
            top, bottom = to_rows(one_class(r, far[0], far[1]))
            ret_send[2 * r] = top
            ret_send[2 * r + 1] = bottom
        for d in range(1, subs):
            to = lax.rem(s + d, subs)
            copy = pltpu.make_async_remote_copy(
                src_ref=ret_send.at[to // 2],
                dst_ref=ret_sub.at[s],
                send_sem=send_sem.at[16 + 4 + d],
                recv_sem=recv_sem.at[16 + 4 + d],
                device_id=peer_sub(d),
                device_id_type=pl.DeviceIdType.MESH,
            )
            copy.start()
            back.append(copy)
        ret_sub[s] = ret_send[s // 2]

    patch_class(3)
    group_classes()
    patch_class(2)
    lax.fori_loop(0, 4, near_group, 0)

    quarter = lane8 >> 5
    blocks = []
    for m in range(8):
        block = None
        for w in range(4):
            part = None
            for r in range(4):
                piece = near[r, pl.ds(32 * m + w + 12 - 2 * r, 8, stride=4), :]
                part = piece if part is None else part + piece
            if w:
                part = pltpu.roll(part, 32 * w, axis=1)
                block = jnp.where(quarter == w, part, block)
            else:
                block = part
        blocks.append(block)
    owned_sums = jnp.concatenate(blocks, axis=0)

    lane_hit, row_hit = [], []
    for j in range(5):
        index = lists[j : j + 1, :]
        column = (index & 127) + ((index >> 12) << 7)
        lane_hit.append(jnp.where(jnp.broadcast_to(column, (256, 128)) == iota((256, 128), 0), 1.0, 0.0).astype(BF16))
        row_hit.append(jnp.broadcast_to((index >> 7) & 31, (32, 128)) == iota((32, 128), 0))

    for copy in back:
        copy.wait()
    returned = None
    for s2 in range(subs):
        returned = ret_sub[s2] if returned is None else returned + ret_sub[s2]
    half = iota((1, 128), 1) >> 6
    returned = jnp.where(half == lax.rem(s, 2), returned, 0.0)
    for copy in back_pat:
        copy.wait()
    for on, taken, onward in relays:
        pl.when(on)(onward.wait_send)
    incoming = [ret_pat[j] for j in range(4)] + [returned]
    left = []
    for j in range(5):
        high = incoming[j].astype(BF16).astype(F32)
        low = incoming[j] - high
        left.append(
            jnp.concatenate(
                [
                    jnp.where(row_hit[j], jnp.broadcast_to(high, (32, 128)), 0.0),
                    jnp.where(row_hit[j], jnp.broadcast_to(low, (32, 128)), 0.0),
                ],
                axis=0,
            ).astype(BF16)
        )
    sums = lax.dot_general(
        jnp.concatenate(left, axis=1), jnp.concatenate(lane_hit, axis=1), NT, preferred_element_type=F32
    )
    sums = sums[0:32] + sums[32:64]
    out_ref[0:32, :] = owned_sums[0:32] + sums[:, 0:128]
    out_ref[32:64, :] = owned_sums[32:64] + sums[:, 128:256]


def per_device(patches, subs, heat, basis, area, corners, send_sub, send_pat, live_faces):
    hbm = pl.BlockSpec(memory_space=pl.ANY)
    out = pl.pallas_call(
        functools.partial(kernel, patches, subs),
        out_shape=pltpu.VMEM((64, 128), F32),
        in_specs=[hbm] * 7,
        out_specs=pl.BlockSpec(memory_space=pltpu.VMEM),
        scratch_shapes=[
            pltpu.SMEM((1,), I32),
            pltpu.VMEM((80, 128), F32),
            pltpu.VMEM((9, 16384), BF16),
            pltpu.VMEM((128, 128), F32),
            pltpu.VMEM((3, 16384), I32),
            pltpu.VMEM((1, 64), I32),
            pltpu.VMEM((4, 128), I32),
            pltpu.VMEM((8, 128), I32),
            pltpu.VMEM((4, 256, 128), I32),
            pltpu.VMEM((4, 256, 128), F32),
            pltpu.VMEM((4, 256, 128), F32),
            pltpu.VMEM((4, 4, 3, 8, 128), I32),
            pltpu.VMEM((4, 4, 3, 8, 128), F32),
            pltpu.VMEM((4, 4, 9, 8, 128), F32),
            pltpu.VMEM((4, 4, 8, 128), F32),
            pltpu.VMEM((4, 4, 4, 3, 8, 128), F32),
            pltpu.VMEM((4, 272, 128), F32),
            pltpu.VMEM((5, 1, 128), F32),
            pltpu.VMEM((8, 1, 128), F32),
            pltpu.VMEM((4, 1, 128), F32),
            pltpu.VMEM((2 * RADIUS, 1, 128), F32),
            pltpu.VMEM((8, 1, 128), F32),
            pltpu.VMEM((8, 1, 128), F32),
            pltpu.VMEM((4, 1, 128), F32),
            pltpu.SemaphoreType.DMA((7,)),
            pltpu.SemaphoreType.DMA((40,)),
            pltpu.SemaphoreType.DMA((40,)),
        ],
        compiler_params=pltpu.CompilerParams(
            collective_id=0, has_side_effects=True, vmem_limit_bytes=32 * 1024 * 1024
        ),
        name="divergence",
    )(
        live_faces,
        *(
            pltpu.with_memory_space_constraint(x, pltpu.HBM)
            for x in (
                heat.reshape(64, 128),
                basis,
                area.reshape(128, 128),
                corners,
                send_sub.reshape(1, 64),
                send_pat,
            )
        )
    )
    return out.reshape(-1)


def solution(mesh):
    placed = (
        P(("patch", "sub")),
        P(None, ("patch", "sub")),
        P(("patch", "sub")),
        P(None, ("patch", "sub")),
        P(("patch", "sub")),
        P(None, ("patch", "sub")),
        P(("patch", "sub")),
    )
    return jax.shard_map(
        functools.partial(per_device, mesh.shape["patch"], mesh.shape["sub"]),
        mesh=mesh,
        in_specs=placed,
        out_specs=P(("patch", "sub")),
        check_vma=False,
    )
```

```python
import functools

import jax
import jax.numpy as jnp
from jax import lax
from jax.experimental import pallas as pl
from jax.experimental.pallas import tpu as pltpu
from jax.sharding import PartitionSpec as P

RADIUS = 2
OFFSETS = [k + 1 for k in range(RADIUS)] + [-(k + 1) for k in range(RADIUS)]
F32 = jnp.float32
BF16 = jnp.bfloat16
I32 = jnp.int32
NT = (((1,), (1,)), ((), ()))
ROW = 8


def lanes_of(table, lane):
    return jnp.take_along_axis(table, lane, axis=1, mode="promise_in_bounds")


def iota(shape, dim):
    return lax.broadcasted_iota(I32, shape, dim)


def kernel(
    patches,
    subs,
    live_hbm,
    heat_hbm,
    basis_hbm,
    area_hbm,
    corners_hbm,
    ssub_hbm,
    spat_hbm,
    out_ref,
    live_ref,
    heat,
    basis,
    area,
    corners,
    ssub,
    spat,
    lists,
    ctile,
    btile,
    blast,
    cgrp,
    vgrp,
    bgrp,
    wgrp,
    rows,
    near,
    fwd_send,
    fwd_sub,
    fwd_pat,
    relay,
    ret_send,
    ret_sub,
    ret_pat,
    in_sem,
    send_sem,
    recv_sem,
):
    p = lax.axis_index("patch")
    s = lax.axis_index("sub")
    owned = 8192

    def peer_sub(d):
        return {"patch": p, "sub": lax.rem(s + d, subs)}

    def peer_pat(offset):
        return {"patch": lax.rem(p + offset + patches, patches), "sub": s}

    barrier = pltpu.get_barrier_semaphore()
    last_row = patches - ROW
    at = lax.rem(p, ROW)
    odd_core = lax.rem(s, 2)
    linked = s + 1 - odd_core
    for offset in OFFSETS:
        to, core = p + offset, s
        if offset > 0:
            to = jnp.where(to >= patches, to - ROW, to)
            core = jnp.where(p + offset >= patches, linked, s)
        pl.semaphore_signal(
            barrier,
            inc=1,
            device_id={"patch": lax.rem(to + patches, patches), "sub": core},
            device_id_type=pl.DeviceIdType.MESH,
        )

    @pl.when((p >= last_row) & (at < RADIUS) & (odd_core == 1))
    def _():
        for back_by in range(2):
            pl.semaphore_signal(
                barrier,
                inc=1,
                device_id={"patch": p - last_row, "sub": s - back_by},
                device_id_type=pl.DeviceIdType.MESH,
            )

    for d in range(1, subs):
        pl.semaphore_signal(barrier, inc=1, device_id=peer_sub(d), device_id_type=pl.DeviceIdType.MESH)

    cp_heat = pltpu.make_async_copy(heat_hbm, heat.at[pl.ds(8, 64)], in_sem.at[0])
    cp_ssub = pltpu.make_async_copy(ssub_hbm, ssub, in_sem.at[1])
    cp_spat = pltpu.make_async_copy(spat_hbm, spat, in_sem.at[2])
    cp_corners = pltpu.make_async_copy(corners_hbm, corners, in_sem.at[3])
    cp_basis = pltpu.make_async_copy(basis_hbm, basis, in_sem.at[4])
    cp_area = pltpu.make_async_copy(area_hbm, area, in_sem.at[5])
    cp_live = pltpu.make_async_copy(live_hbm, live_ref, in_sem.at[6])
    copies = (cp_heat, cp_ssub, cp_spat, cp_corners, cp_basis, cp_area, cp_live)
    for copy in copies:
        copy.start()

    heat[0:8, :] = jnp.zeros((8, 128), F32)
    heat[72:80, :] = jnp.zeros((8, 128), F32)
    for r in range(4):
        near[r, 0:8, :] = jnp.zeros((8, 128), F32)
        near[r, 264:272, :] = jnp.zeros((8, 128), F32)

    cp_heat.wait()
    cp_ssub.wait()
    cp_spat.wait()

    lists[0:4, :] = spat[...]
    one = ssub[...]
    lists[4:5, :] = jnp.concatenate([one, one], axis=1)
    sub8 = iota((8, 128), 0)
    picked = []
    for j in range(5):
        index = jnp.broadcast_to(lists[j : j + 1, :], (8, 128))
        lane = index & 127
        row = index >> 7
        total = jnp.zeros((8, 128), F32)
        for g in range(8):
            values = lanes_of(heat[8 + 8 * g : 16 + 8 * g, :], lane)
            total = jnp.where(row == sub8 + 8 * g, values, total)
        value = jnp.sum(total, axis=0, keepdims=True)
        fwd_send[j] = value
        picked.append(value)

    signals = subs - 1 + 2 * RADIUS
    for k in range(RADIUS):
        over = RADIUS - k
        here = (at == k).astype(I32)
        first_row = (p < ROW).astype(I32)
        signals = signals + here * first_row * (1 - over)
        signals = signals + here * (p >= last_row).astype(I32) * odd_core * 2 * over
    pl.semaphore_wait(barrier, signals)

    forward, relays, starts = [], [], []
    for j, offset in enumerate(OFFSETS):
        copy = pltpu.make_async_remote_copy(
            src_ref=fwd_send.at[j],
            dst_ref=fwd_pat.at[j],
            send_sem=send_sem.at[j],
            recv_sem=recv_sem.at[j],
            device_id=peer_pat(offset),
            device_id_type=pl.DeviceIdType.MESH,
        )
        forward.append(copy)
        if offset > 0:
            starts.append(copy.start)
            continue
        slot = -offset - 1
        over, via = at < -offset, p < -offset
        place = odd_core * RADIUS + slot
        first = pltpu.make_async_remote_copy(
            src_ref=fwd_send.at[j],
            dst_ref=relay.at[place],
            send_sem=send_sem.at[j],
            recv_sem=recv_sem.at[32 + place],
            device_id={"patch": lax.rem(p + last_row, patches), "sub": linked},
            device_id_type=pl.DeviceIdType.MESH,
        )
        starts.append(functools.partial(pl.when(via), first.start))
        starts.append(functools.partial(pl.when(jnp.logical_not(via)), copy.start))
        for kind in range(2):
            on = (odd_core == 1) & over & (p >= last_row)
            place = kind * RADIUS + slot
            hop = {
                "src_ref": relay.at[place],
                "dst_ref": fwd_pat.at[j],
                "send_sem": send_sem.at[32 + place],
                "device_id": {
                    "patch": lax.rem(p + ROW + offset, patches),
                    "sub": s if kind == 1 else s - odd_core,
                },
                "device_id_type": pl.DeviceIdType.MESH,
            }
            taken = pltpu.make_async_remote_copy(**{**hop, "dst_ref": relay.at[place]}, recv_sem=recv_sem.at[32 + place])
            onward = pltpu.make_async_remote_copy(**hop, recv_sem=recv_sem.at[j])
            relays.append((on, taken, onward))
    for on, taken, onward in reversed(relays):

        @pl.when(on)
        def _(taken=taken, onward=onward):
            taken.wait_recv()
            onward.start()

    for start in reversed(starts):
        start()
    for d in range(1, subs):
        copy = pltpu.make_async_remote_copy(
            src_ref=fwd_send.at[4],
            dst_ref=fwd_sub.at[s],
            send_sem=send_sem.at[4 + d],
            recv_sem=recv_sem.at[4 + d],
            device_id=peer_sub(d),
            device_id_type=pl.DeviceIdType.MESH,
        )
        copy.start()
        forward.append(copy)
    fwd_sub[s] = picked[4]

    cp_corners.wait()
    cp_basis.wait()
    cp_area.wait()
    cp_live.wait()

    def relayout(j, carry):
        for r in range(4):
            col = pl.multiple_of(j * 512 + 128 * r, 128)
            row = pl.multiple_of(j * 8, 8)
            ctile[r, pl.ds(row, 3), :] = corners[:, pl.ds(col, 128)]
            block = basis[:, pl.ds(col, 128)].astype(F32)
            btile[r, pl.ds(row, 8), :] = block[0:8]
            blast[r, pl.ds(row, 1), :] = block[8:9]
        return carry

    lax.fori_loop(0, 32, relayout, 0)

    low64 = iota((8, 128), 1) < 64
    lane8 = iota((8, 128), 1)
    a8 = iota((8, 128), 0).astype(F32)
    b32 = iota((32, 128), 0).astype(F32)
    live = live_ref[0]

    def prepare(g, carry):
        base = pl.multiple_of(g * 64, 64)
        first = 8 + 16 * g
        for r in range(4):
            m = first + (r >> 1)
            tab_a = heat[pl.ds(m - 1, 8, stride=2), :]
            tab_b = heat[pl.ds(m, 8, stride=2), :]
            if r & 1:
                tab_a = jnp.where(low64, heat[pl.ds(m + 1, 8, stride=2), :], tab_a)
            for k in range(3):
                corner = ctile[r, pl.ds(base + k, 8, stride=8), :]
                lane = corner & 127
                odd = (corner >> 7) & 1
                cgrp[r, g, k] = corner
                vgrp[r, g, k] = jnp.where(odd == (r >> 1), lanes_of(tab_b, lane), lanes_of(tab_a, lane))
                start = jnp.where(corner >= owned, 248 + 8 * r, sub8 * 8 + (64 * g + 2 * r - 4))
                rows[r, g, 0, k] = ((corner >> 5) - start).astype(F32)
                rows[r, g, 1, k] = (corner & 31).astype(F32)
            for i in range(8):
                bgrp[r, g, i] = btile[r, pl.ds(base + i, 8, stride=8), :]
            bgrp[r, g, 8] = blast[r, pl.ds(base, 8, stride=8), :]
            slot = sub8 * 512 + lane8 + (4096 * g + 128 * r)
            wgrp[r, g] = jnp.where(slot < live, area[pl.ds(32 * g + r, 8, stride=4), :], 0.0)
        return carry

    lax.fori_loop(0, 4, prepare, 0)

    def term_rows(r, g, i, k, places):
        hit = jnp.broadcast_to(rows[r, g, 0, k, i : i + 1, :], (8, 128)) == places
        high = jnp.where(hit, jnp.broadcast_to(rows[r, g, 2, k, i : i + 1, :], (8, 128)), 0.0)
        low = jnp.where(hit, jnp.broadcast_to(rows[r, g, 3, k, i : i + 1, :], (8, 128)), 0.0)
        return jnp.concatenate([high, low], axis=0).astype(BF16)

    def lane_rows(r, g, i, k):
        hit = jnp.broadcast_to(rows[r, g, 1, k, i : i + 1, :], (32, 128)) == b32
        return jnp.where(hit, 1.0, 0.0).astype(BF16)

    def one_class(r, far0, far1):
        for g in range(4):
            values = []
            for k in range(3):
                corner = cgrp[r, g, k]
                lane = corner & 127
                far_value = jnp.where(((corner >> 7) & 1) == 1, lanes_of(far1, lane), lanes_of(far0, lane))
                values.append(jnp.where(corner >= owned, far_value, vgrp[r, g, k]))
            bas = [bgrp[r, g, i] for i in range(9)]
            grad = [bas[c] * values[0] + bas[3 + c] * values[1] + bas[6 + c] * values[2] for c in range(3)]
            square = grad[0] * grad[0] + grad[1] * grad[1] + grad[2] * grad[2]
            scale = -wgrp[r, g] * lax.rsqrt(jnp.maximum(square, 1.0))
            for k in range(3):
                term = (bas[3 * k] * grad[0] + bas[3 * k + 1] * grad[1] + bas[3 * k + 2] * grad[2]) * scale
                high = term.astype(BF16).astype(F32)
                rows[r, g, 2, k] = high
                rows[r, g, 3, k] = term - high
        far_sum = jnp.zeros((8, 32), F32)
        for g in range(4):
            left, right = [], []
            for i in range(8):
                for k in range(3):
                    left.append(term_rows(r, g, i, k, a8 + 8.0))
                    right.append(lane_rows(r, g, i, k))
            sums = lax.dot_general(
                jnp.concatenate(left, axis=1), jnp.concatenate(right, axis=1), NT, preferred_element_type=F32
            )
            far_sum = far_sum + (sums[0:8] + sums[8:16])
        return far_sum

    def near_group(g, carry):
        for r in range(4):
            for i in range(8):
                sums = lax.dot_general(
                    jnp.concatenate([term_rows(r, g, i, k, a8) for k in range(3)], axis=1),
                    jnp.concatenate([lane_rows(r, g, i, k) for k in range(3)], axis=1),
                    NT,
                    preferred_element_type=F32,
                )
                near[r, pl.ds(pl.multiple_of(8 + 64 * g + 8 * i, 8), 8), 0:32] = sums[0:8] + sums[8:16]
        return carry

    def to_rows(far_sum):
        wide = jnp.concatenate([far_sum, jnp.zeros((8, 96), F32)], axis=1)
        total = jnp.where((sub8 & 3) == 0, wide, 0.0)
        for w in range(1, 4):
            total = jnp.where((sub8 & 3) == w, pltpu.roll(wide, 32 * w, axis=1), total)
        return jnp.sum(total[0:4], axis=0, keepdims=True), jnp.sum(total[4:8], axis=0, keepdims=True)

    def wide_rows(row):
        return jnp.broadcast_to(row, (8, 128))

    back, back_pat = [], []

    def sums_back(j):
        return pltpu.make_async_remote_copy(
            src_ref=ret_send.at[4 + j],
            dst_ref=ret_pat.at[j],
            send_sem=send_sem.at[16 + j],
            recv_sem=recv_sem.at[16 + j],
            device_id=peer_pat(-OFFSETS[j]),
            device_id_type=pl.DeviceIdType.MESH,
        )

    def patch_class(r):
        far = []
        for q in range(2):
            forward[2 * (r - 2) + q].wait()
            far.append(wide_rows(fwd_pat[2 * (r - 2) + q]))
        for q, row in enumerate(to_rows(one_class(r, far[0], far[1]))):
            j = 2 * (r - 2) + q
            ret_send[2 * r + q] = row
            sums_back(j).start()

    def group_classes():
        low_row = iota((1, 128), 1) < 64
        for copy in forward[4:]:
            copy.wait()
        for r in range(2):
            far = []
            for q in range(2):
                far.append(wide_rows(jnp.where(low_row, fwd_sub[4 * r + 2 * q], fwd_sub[4 * r + 2 * q + 1])))
            top, bottom = to_rows(one_class(r, far[0], far[1]))
            ret_send[2 * r] = top
            ret_send[2 * r + 1] = bottom
        for d in range(1, subs):
            to = lax.rem(s + d, subs)
            copy = pltpu.make_async_remote_copy(
                src_ref=ret_send.at[to // 2],
                dst_ref=ret_sub.at[s],
                send_sem=send_sem.at[16 + 4 + d],
                recv_sem=recv_sem.at[16 + 4 + d],
                device_id=peer_sub(d),
                device_id_type=pl.DeviceIdType.MESH,
            )
            copy.start()
            back.append(copy)
        ret_sub[s] = ret_send[s // 2]

    pl.when(p > 0)(functools.partial(patch_class, 3))
    group_classes()
    pl.when(p == 0)(functools.partial(patch_class, 3))
    patch_class(2)
    back_pat.extend(sums_back(j) for j in (2, 3, 0, 1))
    lax.fori_loop(0, 4, near_group, 0)

    quarter = lane8 >> 5
    blocks = []
    for m in range(8):
        block = None
        for w in range(4):
            part = None
            for r in range(4):
                piece = near[r, pl.ds(32 * m + w + 12 - 2 * r, 8, stride=4), :]
                part = piece if part is None else part + piece
            if w:
                part = pltpu.roll(part, 32 * w, axis=1)
                block = jnp.where(quarter == w, part, block)
            else:
                block = part
        blocks.append(block)
    owned_sums = jnp.concatenate(blocks, axis=0)

    lane_hit, row_hit = [], []
    for j in range(5):
        index = lists[j : j + 1, :]
        column = (index & 127) + ((index >> 12) << 7)
        lane_hit.append(jnp.where(jnp.broadcast_to(column, (256, 128)) == iota((256, 128), 0), 1.0, 0.0).astype(BF16))
        row_hit.append(jnp.broadcast_to((index >> 7) & 31, (32, 128)) == iota((32, 128), 0))

    for copy in back:
        copy.wait()
    returned = None
    for s2 in range(subs):
        returned = ret_sub[s2] if returned is None else returned + ret_sub[s2]
    half = iota((1, 128), 1) >> 6
    returned = jnp.where(half == lax.rem(s, 2), returned, 0.0)
    for copy in back_pat:
        copy.wait()
    for on, taken, onward in relays:
        pl.when(on)(onward.wait_send)
    incoming = [ret_pat[j] for j in range(4)] + [returned]
    left = []
    for j in range(5):
        high = incoming[j].astype(BF16).astype(F32)
        low = incoming[j] - high
        left.append(
            jnp.concatenate(
                [
                    jnp.where(row_hit[j], jnp.broadcast_to(high, (32, 128)), 0.0),
                    jnp.where(row_hit[j], jnp.broadcast_to(low, (32, 128)), 0.0),
                ],
                axis=0,
            ).astype(BF16)
        )
    sums = lax.dot_general(
        jnp.concatenate(left, axis=1), jnp.concatenate(lane_hit, axis=1), NT, preferred_element_type=F32
    )
    sums = sums[0:32] + sums[32:64]
    out_ref[0:32, :] = owned_sums[0:32] + sums[:, 0:128]
    out_ref[32:64, :] = owned_sums[32:64] + sums[:, 128:256]


def per_device(patches, subs, heat, basis, area, corners, send_sub, send_pat, live_faces):
    hbm = pl.BlockSpec(memory_space=pl.ANY)
    out = pl.pallas_call(
        functools.partial(kernel, patches, subs),
        out_shape=pltpu.VMEM((64, 128), F32),
        in_specs=[hbm] * 7,
        out_specs=pl.BlockSpec(memory_space=pltpu.VMEM),
        scratch_shapes=[
            pltpu.SMEM((1,), I32),
            pltpu.VMEM((80, 128), F32),
            pltpu.VMEM((9, 16384), BF16),
            pltpu.VMEM((128, 128), F32),
            pltpu.VMEM((3, 16384), I32),
            pltpu.VMEM((1, 64), I32),
            pltpu.VMEM((4, 128), I32),
            pltpu.VMEM((8, 128), I32),
            pltpu.VMEM((4, 256, 128), I32),
            pltpu.VMEM((4, 256, 128), F32),
            pltpu.VMEM((4, 256, 128), F32),
            pltpu.VMEM((4, 4, 3, 8, 128), I32),
            pltpu.VMEM((4, 4, 3, 8, 128), F32),
            pltpu.VMEM((4, 4, 9, 8, 128), F32),
            pltpu.VMEM((4, 4, 8, 128), F32),
            pltpu.VMEM((4, 4, 4, 3, 8, 128), F32),
            pltpu.VMEM((4, 272, 128), F32),
            pltpu.VMEM((5, 1, 128), F32),
            pltpu.VMEM((8, 1, 128), F32),
            pltpu.VMEM((4, 1, 128), F32),
            pltpu.VMEM((2 * RADIUS, 1, 128), F32),
            pltpu.VMEM((8, 1, 128), F32),
            pltpu.VMEM((8, 1, 128), F32),
            pltpu.VMEM((4, 1, 128), F32),
            pltpu.SemaphoreType.DMA((7,)),
            pltpu.SemaphoreType.DMA((40,)),
            pltpu.SemaphoreType.DMA((40,)),
        ],
        compiler_params=pltpu.CompilerParams(
            collective_id=0, has_side_effects=True, vmem_limit_bytes=32 * 1024 * 1024
        ),
        name="divergence",
    )(
        live_faces,
        *(
            pltpu.with_memory_space_constraint(x, pltpu.HBM)
            for x in (
                heat.reshape(64, 128),
                basis,
                area.reshape(128, 128),
                corners,
                send_sub.reshape(1, 64),
                send_pat,
            )
        )
    )
    return out.reshape(-1)


def solution(mesh):
    placed = (
        P(("patch", "sub")),
        P(None, ("patch", "sub")),
        P(("patch", "sub")),
        P(None, ("patch", "sub")),
        P(("patch", "sub")),
        P(None, ("patch", "sub")),
        P(("patch", "sub")),
    )
    return jax.shard_map(
        functools.partial(per_device, mesh.shape["patch"], mesh.shape["sub"]),
        mesh=mesh,
        in_specs=placed,
        out_specs=P(("patch", "sub")),
        check_vma=False,
    )
```
